32 devices in a mesh: group: 8 (over y, x, core), expert: 4 (over z).
Axes of the slice: x: 2, y: 2, z: 4, core: 2. Of those that a mesh axis runs over, the one named last changes fastest.
Arguments:
- tokens: bfloat16 [8192, 2048], P(('group', 'expert')), may hold values from -6 to 6
- routes: int32 [8192, 8], P(('group', 'expert')), may hold values from 0 to 15, all different within a row; in each aligned block of 256 rows (0 to 255, 256 to 511, ...) at most 256 rows name the same one
- prefix: int32 [8], P('group'), may hold values from 102 to 512
- query_weight: float32 [2048, 2048], P('group'), may hold values from -0.125 to 0.125
- key_weight: float32 [2048, 2048], P('group'), may hold values from -0.125 to 0.125
- value_weight: float32 [2048, 2048], P('group'), may hold values from -0.125 to 0.125
- output_weight: float32 [2048, 2048], P('group'), may hold values from -1 to 1
- router_weight: float32 [2048, 16], P('group'), may hold values from -0.0625 to 0.0625
- attention_gain: float32 [2048], P('group'), may hold values from 0.5 to 1.5
- feedforward_gain: float32 [2048], P('group'), may hold values from 0.5 to 1.5
- query_gain: float32 [2048], P('group'), may hold values from 0.8 to 1.6
- key_gain: float32 [2048], P('group'), may hold values from 0.8 to 1.6
- expert_in: float32 [2048, 16, 2048], P('group', 'expert'), may hold values from -0.125 to 0.125
- expert_down: float32 [1024, 16, 2048], P('group', 'expert'), may hold values from -1.75 to 1.75
- cotangent: bfloat16 [8192, 2048], P(('group', 'expert')), may hold values from -6 to 6
Outputs:
- output: bfloat16 [8192, 2048], P(('group', 'expert'))
- grad_tokens: float32 [8192, 2048], P(('group', 'expert'))
- grad_query: float32 [2048, 2048], P('group')
- grad_key: float32 [2048, 2048], P('group')
- grad_value: float32 [2048, 2048], P('group')
- grad_output: float32 [2048, 2048], P('group')
- grad_router: float32 [2048, 16], P('group')
- grad_attention_gain: float32 [2048], P('group')
- grad_feedforward_gain: float32 [2048], P('group')
- grad_query_gain: float32 [2048], P('group')
- grad_key_gain: float32 [2048], P('group')
- grad_expert_in: float32 [2048, 16, 2048], P('group', 'expert')
- grad_expert_down: float32 [1024, 16, 2048], P('group', 'expert')
The draws below stay inside these ranges and needn't reach their ends.
Inputs may be any that keep to these rules, and one draw needn't show every extreme that they name: `routes`: in each aligned block of 256 rows (the rows of one device) no expert is named by more than 256 rows, and in some block one expert is named by exactly 256 rows; the 8 experts of a row differ.
All inputs are finite; a program needn't handle non-finite values.
Results may differ from the reference program's by a relative error of at most 0.025.
Values may be sent and summed in bfloat16 or wider, within the bound.
A program may use at most 448 MiB of HBM per device.

```python
import math
import jax
import jax.numpy as jnp
import numpy as np
from jax import lax

D = 2048
HEADS = 16
HEAD_DIM = 128
FF = 1024
TOP = 8
LEN = 1024
SEQS = 1
EXPERTS = 16
NSEQ = 8
SLICE = 256
TOK_DEV = 256
TOKENS = 8192
CAP = 256
N_GROUP = 8
N_EXPERT = 4


def place_ends(drawn, key, least, top_value):
    longest = drawn.shape.index(max(drawn.shape))
    spots = []
    for shift in (0, 1):
        where = [jax.random.randint(jax.random.fold_in(key, axis), (), 0, length) for axis, length in enumerate(drawn.shape)]
        where[longest] = (where[longest] + shift) % drawn.shape[longest]
        spots.append(tuple(where))
    return drawn.at[spots[0]].set(least).at[spots[1]].set(top_value)


def with_spikes(values, rng, source, target, blocks, factor):
    owner, partner = [(jnp.arange(values.shape[dim]) // (values.shape[dim] // blocks)).reshape([-1 if axis == dim else 1 for axis in range(values.ndim)]) for dim in (source, target)]
    chosen = jax.random.permutation(rng, blocks)[partner]
    strong = (owner == chosen) | (owner == (partner + blocks // 2) % blocks)
    return jnp.where(strong, factor * values, values)


def level_of(rng, dims, cuts, low, high):
    gain = 1.0
    for axis_at, blocks in cuts:
        draws = jax.random.uniform(jax.random.fold_in(jax.random.fold_in(rng, 6), axis_at), (blocks,), jnp.float32, low / len(cuts), high / len(cuts))
        gain = gain * jnp.repeat(jnp.exp(draws), dims[axis_at] // blocks).reshape((-1,) + (1,) * (len(dims) - 1 - axis_at))
    return gain


def deal_out(own_key, own, number, rows, number_of, top, bound, skew):
    ranking = jax.random.permutation(own_key, number_of)
    heavy_load, ordinary = portions_of(number_of, rows * top, bound, skew, True), portions_of(number_of, rows * top, bound, skew, False)
    places = jnp.arange(number_of)

    def named(lengths, offset_by):
        used = int((lengths > 0).sum())
        fixed = max(1, used // 4)
        shifted = fixed + (places - fixed + offset_by * (used - fixed)) % max(1, number_of - fixed)
        return jnp.zeros((number_of,), jnp.int32).at[ranking[jnp.where(places < fixed, places, shifted)]].set(jnp.asarray(lengths, jnp.int32))

    lengths = jnp.where(number % 4 == 0, named(heavy_load, number // 4), named(ordinary, number - number // 4 - 1))
    mixed = jax.random.permutation(jax.random.fold_in(own, 3), number_of)
    donor, receiver = mixed[0:number_of // 2 * 2:2], mixed[1:number_of // 2 * 2:2]
    room = jnp.minimum(lengths[donor] - 1, bound - lengths[receiver]) // 2
    room = jnp.where((donor == ranking[0]) | (receiver == ranking[0]) | (lengths[receiver] == 0), 0, jnp.maximum(room, 0))
    shifted = jax.random.randint(jax.random.fold_in(own, 4), (number_of // 2,), 0, 1 << 20) % (room + 1)
    lengths = lengths.at[donor].add(-shifted).at[receiver].add(shifted)
    labels = jnp.searchsorted(jnp.cumsum(lengths), jnp.arange(rows * top), side="right").astype(jnp.int32)
    grid = labels.reshape(top, rows).T
    grid = grid[jax.random.permutation(jax.random.fold_in(own, 1), rows)]
    offset_by = jax.random.randint(jax.random.fold_in(own, 2), (rows, 1), 0, top)
    return jnp.take_along_axis(grid, (jnp.arange(top)[None, :] + offset_by) % top, axis=1)


def portions_of(number_of, total, limit, slope, full):
    weights = [(1 << 20) // math.isqrt(rank ** slope) + 1 for rank in range(1, number_of + 1)]
    largest = limit if full else min(limit, max(-(-total // number_of), total * weights[0] // sum(weights)))
    least = 1 if total - largest >= number_of - 1 else 0
    given, rest = [largest] + [least] * (number_of - 1), total - largest - least * (number_of - 1)
    while rest > 0:
        movable = [i for i in range(1, number_of) if given[i] < largest] or [i for i in range(1, number_of) if given[i] < limit]
        mass, remaining = sum([weights[i] for i in movable]), rest
        for i in movable:
            extra = min(limit - given[i], max(1, remaining * weights[i] // mass), rest)
            given[i] = given[i] + extra
            rest = rest - extra
    return np.array(given)


def bell_draw(key, dims, width, reach, shards=(), dtype=jnp.bfloat16):
    array = width * jax.random.normal(key, dims, jnp.float32)
    if shards:
        array = array * level_of(key, dims, shards, -0.22, 0.18)
    return jnp.clip(array, -reach, reach).astype(dtype)


def noise_with(key, dims, width, bound, split, heavy, dtype=jnp.bfloat16):
    drawn = width * jax.random.normal(key, dims, jnp.float32)
    if split:
        drawn = drawn * level_of(key, dims, split, -0.22, 0.18)
    return jnp.clip(with_spikes(drawn, jax.random.fold_in(key, 3), *heavy), -bound, bound).astype(dtype)


def setup_inputs(seed: int = 0) -> dict:
    splits = jax.random.split(jax.random.key(seed), 16)
    tokens = bell_draw(splits[0], (TOKENS, D), 1.0, 6.0, ((0, 32),))
    routes_keys = jax.random.split(jax.random.fold_in(splits[1], 1), TOKENS // TOK_DEV)
    routes_turns = jax.random.permutation(jax.random.fold_in(splits[1], 3), TOKENS // TOK_DEV)
    routes = jax.vmap(lambda own, number: deal_out(jax.random.fold_in(splits[1], 2), own, number, TOK_DEV, EXPERTS, TOP, CAP, 1))(routes_keys, routes_turns).reshape((TOKENS, TOP))
    prefix = place_ends(jax.random.randint(splits[2], (NSEQ,), LEN // 10, LEN // 2 + 1), jax.random.fold_in(splits[2], 1), LEN // 10, (LEN // 2 + 1) - 1).astype(jnp.int32)
    query_weight = bell_draw(splits[3], (D, D), D ** -0.5, 0.125, ((0, 8),), jnp.float32)
    key_weight = bell_draw(splits[4], (D, D), D ** -0.5, 0.125, ((0, 8),), jnp.float32)
    value_weight = bell_draw(splits[5], (D, D), D ** -0.5, 0.125, ((0, 8),), jnp.float32)
    output_weight = bell_draw(splits[6], (D, D), (D // 64) ** -0.5, 1.0, ((0, 8),), jnp.float32)
    router_weight = bell_draw(splits[7], (D, EXPERTS), (4 * D) ** -0.5, 0.0625, ((0, 8),), jnp.float32)
    attention_gain = jnp.clip(1.0 + 0.1 * jax.random.normal(splits[8], (D,), jnp.float32), 0.5, 1.5)
    feedforward_gain = jnp.clip(1.0 + 0.1 * jax.random.normal(splits[9], (D,), jnp.float32), 0.5, 1.5)
    query_gain = jnp.clip(0.8 + 0.8 * jax.random.uniform(splits[10], (D,), jnp.float32) ** level_of(splits[10], (D,), ((0, 8),), -0.2, 0.2), 0.8, 1.6)
    key_gain = jnp.clip(0.8 + 0.8 * jax.random.uniform(splits[11], (D,), jnp.float32) ** level_of(splits[11], (D,), ((0, 8),), -0.2, 0.2), 0.8, 1.6)
    expert_in = bell_draw(splits[12], (D, EXPERTS, 2 * FF), D ** -0.5, 0.125, ((0, 8), (1, 4)), jnp.float32)
    expert_down = bell_draw(splits[13], (FF, EXPERTS, D), (max(1, 3 * FF // (EXPERTS * EXPERTS))) ** -0.5, 1.75, ((0, 8), (1, 4)), jnp.float32)
    cotangent = noise_with(splits[14], (TOKENS, D), 1.0, 6.0, ((0, 32),), (0, 1, 32, 2.75))
    return dict(tokens=tokens, routes=routes, prefix=prefix, query_weight=query_weight, key_weight=key_weight, value_weight=value_weight, output_weight=output_weight, router_weight=router_weight, attention_gain=attention_gain, feedforward_gain=feedforward_gain, query_gain=query_gain, key_gain=key_gain, expert_in=expert_in, expert_down=expert_down, cotangent=cotangent)


EPS = 1e-05
THETA = 10000.0
HIGH = lax.Precision.HIGHEST

@jax.custom_vjp
def low(v):
    return lax.optimization_barrier(v.astype(jnp.bfloat16)).astype(jnp.float32)

@jax.custom_vjp
def low_back(v):
    return v

def low_keep(v):
    return (low(v), None)

def low_pass(kept, grad):
    return (grad,)

def back_keep(v):
    return (v, None)

def back_low(kept, grad):
    return (low(grad),)
low.defvjp(low_keep, low_pass)
low_back.defvjp(back_keep, back_low)

def normed(values):
    return values * lax.rsqrt(lax.optimization_barrier(jnp.mean(values * values, -1, keepdims=True)) + EPS)

def rope_tables(positions):
    steps = jnp.arange(HEAD_DIM // 2).astype(jnp.float32)
    freq = jnp.exp(steps * (-2.0 * math.log(THETA) / HEAD_DIM))
    angle = positions[:, None] * freq[None, :]
    return (jnp.cos(angle)[:, None, :], jnp.sin(angle)[:, None, :])

def rotate(values, cosine, sine):
    half = values.shape[-1] // 2
    first = values[..., :half]
    second = values[..., half:]
    return jnp.concatenate([first * cosine - second * sine, second * cosine + first * sine], -1)

def to_seq(values):
    return values.reshape(N_GROUP, N_EXPERT, SEQS, SLICE, -1).transpose(0, 2, 1, 3, 4).reshape(NSEQ, LEN, -1)

def from_seq(values):
    return values.reshape(N_GROUP, SEQS, N_EXPERT, SLICE, -1).transpose(0, 2, 1, 3, 4).reshape(TOKENS, -1)

def attend_one(pieces):
    query, key, value, prefix_len = pieces
    scores = low_back(jnp.einsum('qhd,khd->hqk', query, key, precision=HIGH))
    rows_at = jnp.arange(LEN).astype(jnp.int32)[:, None]
    cols_at = jnp.arange(LEN).astype(jnp.int32)[None, :]
    allowed = (cols_at <= rows_at) | (cols_at < prefix_len)
    masked = jnp.where(allowed[None], scores, -1e+30)
    weights = low(jax.nn.softmax(masked, -1))
    result = jnp.einsum('hqk,khd->qhd', weights, value, precision=HIGH)
    return result.reshape(LEN, D)

def forward(xfloat, query_weight, key_weight, value_weight, output_weight, router_weight, attention_gain, feedforward_gain, query_gain, key_gain, expert_in, expert_down, prefix, table, selected):
    hidden_one = low(normed(xfloat) * low(attention_gain))
    query_lin = low_back(jnp.dot(hidden_one, low(query_weight), precision=HIGH))
    key_lin = low_back(jnp.dot(hidden_one, low(key_weight), precision=HIGH))
    values = low_back(low(jnp.dot(hidden_one, low(value_weight), precision=HIGH)))
    query_normed = normed(query_lin) * low(query_gain)
    key_normed = normed(key_lin) * low(key_gain)
    cosine, sine = rope_tables(jnp.arange(LEN).astype(jnp.float32))
    query_seq = to_seq(query_normed).reshape(NSEQ, LEN, HEADS, HEAD_DIM)
    key_seq = to_seq(key_normed).reshape(NSEQ, LEN, HEADS, HEAD_DIM)
    value_seq = to_seq(values).reshape(NSEQ, LEN, HEADS, HEAD_DIM)
    query_seq = low(rotate(query_seq, cosine, sine) * HEAD_DIM ** (-0.5))
    key_seq = low(rotate(key_seq, cosine, sine))
    attended = lax.map(jax.checkpoint(attend_one), (query_seq, key_seq, value_seq, prefix))
    attended = low_back(low(from_seq(attended)))
    attn_out = low_back(jnp.dot(attended, low(output_weight), precision=HIGH))
    resid = xfloat + attn_out
    hidden_two = low(normed(resid) * low(feedforward_gain))
    logits = low_back(jnp.dot(hidden_two, low(router_weight), precision=HIGH))
    weights = jax.nn.softmax(logits, -1) * selected
    padded_rows = jnp.concatenate([hidden_two, jnp.zeros((1, D), jnp.float32)], 0)
    padded_weights = jnp.concatenate([weights, jnp.zeros((1, EXPERTS), jnp.float32)], 0)

    def expert_step(total, pieces):
        table_row, weight_in, weight_down, weight_col = pieces
        rows_in = low_back(padded_rows[table_row])
        both = low_back(jnp.dot(rows_in, weight_in, precision=HIGH))
        gate_part = both[:, :FF]
        up_part = both[:, FF:]
        hidden = low(jax.nn.silu(gate_part) * up_part)
        result = low_back(low(jnp.dot(hidden, weight_down, precision=HIGH)))
        return (total.at[table_row].add(weight_col[table_row][:, None] * result), None)
    initial = jnp.zeros((TOKENS + 1, D), jnp.float32)
    total, unused = lax.scan(jax.checkpoint(expert_step), initial, (table, jnp.moveaxis(low(expert_in), 1, 0), jnp.moveaxis(low(expert_down), 1, 0), padded_weights.T))
    return resid + total[:TOKENS]

def reference(tokens, routes, prefix, query_weight, key_weight, value_weight, output_weight, router_weight, attention_gain, feedforward_gain, query_gain, key_gain, expert_in, expert_down, cotangent):
    blocks_all = N_GROUP * N_EXPERT
    onehot = (routes[:, :, None] == jnp.arange(EXPERTS).astype(jnp.int32)[None, None, :]).astype(jnp.int32)
    blocked = onehot.reshape(blocks_all, TOK_DEV * TOP, EXPERTS)
    before = jnp.cumsum(blocked, 1) - blocked
    slots = lax.optimization_barrier(jnp.sum(before * blocked, -1)).reshape(TOKENS, TOP).astype(jnp.int32)
    token_ids = jnp.broadcast_to(jnp.arange(TOKENS).astype(jnp.int32)[:, None], (TOKENS, TOP))
    places = routes * (blocks_all * CAP) + token_ids // TOK_DEV * CAP + slots
    table = jnp.full((EXPERTS * blocks_all * CAP,), TOKENS, jnp.int32)
    table = table.at[places.reshape(-1)].set(token_ids.reshape(-1)).reshape(EXPERTS, blocks_all * CAP)
    selected = lax.optimization_barrier(jnp.sum(onehot, 1)).astype(jnp.float32)
    xfloat = tokens.astype(jnp.float32)

    def closed(xvalue, wq, wk, wv, wo, wr, ga, gf, gq, gk, win, wdown):
        return forward(xvalue, wq, wk, wv, wo, wr, ga, gf, gq, gk, win, wdown, prefix, table, selected)
    primal, pullback = jax.vjp(closed, xfloat, query_weight, key_weight, value_weight, output_weight, router_weight, attention_gain, feedforward_gain, query_gain, key_gain, expert_in, expert_down)
    grads = pullback(cotangent.astype(jnp.float32))
    return (primal.astype(jnp.bfloat16), grads[0], grads[1], grads[2], grads[3], grads[4], grads[5], grads[6], grads[7], grads[8], grads[9], grads[10], grads[11])
```

```python
import functools
import math

import jax
import jax.numpy as jnp
from jax import lax
from jax.experimental import pallas as pl
from jax.experimental.pallas import tpu as pltpu
from jax.sharding import PartitionSpec as P

HEADS = 16
HEAD_DIM = 128
LEN = 1024
MAX_PREFIX = LEN // 2
QBLOCK = 256
EPS = 1e-05
THETA = 10000.0
BF = jnp.bfloat16
F32 = jnp.float32


def dot(left, right):
    return jnp.dot(left, right, preferred_element_type=F32)


def dot_nt(left, right):
    return lax.dot_general(left, right, (((1,), (1,)), ((), ())), preferred_element_type=F32)


def dot_tn(left, right):
    return lax.dot_general(left, right, (((0,), (0,)), ((), ())), preferred_element_type=F32)


def row_scale(values):
    return lax.rsqrt(jnp.mean(values * values, -1, keepdims=True) + EPS)


def norm_back(values, scale_rows, upstream):
    inner = jnp.mean(upstream * values, -1, keepdims=True)
    return scale_rows * upstream - values * (scale_rows * scale_rows * scale_rows) * inner


def shift(value, count, step):
    return lax.ppermute(value, "expert", [(i, (i + step) % count) for i in range(count)])


def ring_gather(value, count, here):
    rows = value.shape[0]
    whole = jnp.zeros((count * rows,) + value.shape[1:], value.dtype)
    for step in range(count):
        if step:
            value = shift(value, count, 1)
        whole = lax.dynamic_update_slice(whole, value, (((here - step) % count) * rows, 0))
    return whole


def ring_scatter(term, count, here):
    total = term((here - 1) % count)
    for step in range(1, count):
        arrived = shift(total.astype(BF), count, 1)
        total = term((here - 1 - step) % count) + arrived.astype(F32)
    return total


def exchange_sum(value, count):
    total = value
    for step in range(1, count):
        total = total + shift(value, count, step)
    return total


def key_limit(block):
    return max((block + 1) * QBLOCK, MAX_PREFIX)


def visible(block, limit, prefix):
    row = block * QBLOCK + lax.broadcasted_iota(jnp.int32, (QBLOCK, limit), 0)
    col = lax.broadcasted_iota(jnp.int32, (QBLOCK, limit), 1)
    return (col <= row) | (col < prefix)


def attend_kernel(prefix_ref, ql, kl, vb, sq, sk, gq, gk, cos, sin, ob, qb, kb, lse):
    prefix = prefix_ref[0]
    c, s = cos[...], sin[...]
    qn = ql[...] * sq[...] * gq[...]
    kn = kl[...] * sk[...] * gk[...]
    half = HEAD_DIM // 2
    qb[...] = ((qn * c + pltpu.roll(qn, half, 1) * s) * HEAD_DIM ** (-0.5)).astype(BF)
    kb[...] = (kn * c + pltpu.roll(kn, half, 1) * s).astype(BF)
    for block in range(LEN // QBLOCK):
        rows = slice(block * QBLOCK, (block + 1) * QBLOCK)
        limit = key_limit(block)
        scores = dot_nt(qb[rows, :], kb[:limit, :])
        scores = jnp.where(visible(block, limit, prefix), scores, -1e30)
        peak = jnp.max(scores, -1, keepdims=True)
        expo = jnp.exp(scores - peak)
        total = jnp.sum(expo, -1, keepdims=True)
        ob[rows, :] = (dot(expo.astype(BF), vb[:limit, :]) / total).astype(BF)
        lse[0, rows, :] = peak + jnp.log(total)


def attend(prefix, ql, kl, vb, sq, sk, gq, gk, cos, sin):
    heads = ql.shape[1] // HEAD_DIM
    col = pl.BlockSpec((LEN, HEAD_DIM), lambda h, p: (0, h))
    one = pl.BlockSpec((LEN, 1), lambda h, p: (0, 0))
    gain = pl.BlockSpec((1, HEAD_DIM), lambda h, p: (0, h))
    table = pl.BlockSpec((LEN, HEAD_DIM), lambda h, p: (0, 0))
    return pl.pallas_call(
        attend_kernel,
        out_shape=[jax.ShapeDtypeStruct(ql.shape, BF)] * 3
        + [jax.ShapeDtypeStruct((heads, LEN, 1), F32)],
        grid_spec=pltpu.PrefetchScalarGridSpec(
            num_scalar_prefetch=1,
            grid=(heads,),
            in_specs=[col, col, col, one, one, gain, gain, table, table],
            out_specs=[col, col, col, pl.BlockSpec((1, LEN, 1), lambda h, p: (h, 0, 0))],
        ),
        cost_estimate=pl.CostEstimate(
            flops=heads * LEN * LEN * HEAD_DIM * 3, bytes_accessed=16 << 20, transcendentals=heads * LEN * LEN
        ),
        name="attend",
    )(prefix, ql, kl, vb, sq, sk, gq, gk, cos, sin)


def attend_back_kernel(
    prefix_ref, qb, kb, vb, dob, lse, ql, kl, sq, sk, gq, gk, cos, sin,
    wq, wk, dv, inner, gain_q, gain_k, dq_sum, dk_sum, dv_sum,
):
    prefix = prefix_ref[0]
    dk_sum[...] = jnp.zeros_like(dk_sum)
    dv_sum[...] = jnp.zeros_like(dv_sum)
    for block in range(LEN // QBLOCK):
        rows = slice(block * QBLOCK, (block + 1) * QBLOCK)
        limit = key_limit(block)
        scores = dot_nt(qb[rows, :], kb[:limit, :])
        weights = jnp.where(visible(block, limit, prefix), jnp.exp(scores - lse[0, rows, :]), 0.0)
        grad = dob[rows, :]
        dweights = dot_nt(grad, vb[:limit, :])
        dscores = (weights * (dweights - jnp.sum(dweights * weights, -1, keepdims=True))).astype(BF)
        dq_sum[rows, :] = dot(dscores, kb[:limit, :])
        dk_sum[:limit, :] += dot_tn(dscores, qb[rows, :])
        dv_sum[:limit, :] += dot_tn(weights.astype(BF), grad)
    dv[...] = dv_sum[...].astype(BF)
    c, s = cos[...], sin[...]
    half = HEAD_DIM // 2
    dq = dq_sum[...] * HEAD_DIM ** (-0.5)
    dqn = dq * c - pltpu.roll(dq, half, 1) * s
    dk = dk_sum[...]
    dkn = dk * c - pltpu.roll(dk, half, 1) * s
    gain_q[...] = jnp.sum(dqn * (ql[...] * sq[...]), 0, keepdims=True)
    gain_k[...] = jnp.sum(dkn * (kl[...] * sk[...]), 0, keepdims=True)
    dqn = dqn * gq[...]
    dkn = dkn * gk[...]
    wq[...] = dqn
    wk[...] = dkn
    part = jnp.concatenate(
        [jnp.sum(dqn * ql[...], -1, keepdims=True), jnp.sum(dkn * kl[...], -1, keepdims=True)], 1
    )

    @pl.when(pl.program_id(0) == 0)
    def _():
        inner[...] = part

    @pl.when(pl.program_id(0) > 0)
    def _():
        inner[...] += part


def attend_back(prefix, qb, kb, vb, dob, lse, ql, kl, sq, sk, gq, gk, cos, sin):
    heads = ql.shape[1] // HEAD_DIM
    col = pl.BlockSpec((LEN, HEAD_DIM), lambda h, p: (0, h))
    one = pl.BlockSpec((LEN, 1), lambda h, p: (0, 0))
    gain = pl.BlockSpec((1, HEAD_DIM), lambda h, p: (0, h))
    table = pl.BlockSpec((LEN, HEAD_DIM), lambda h, p: (0, 0))
    return pl.pallas_call(
        attend_back_kernel,
        out_shape=[
            jax.ShapeDtypeStruct(ql.shape, F32),
            jax.ShapeDtypeStruct(ql.shape, F32),
            jax.ShapeDtypeStruct(ql.shape, BF),
            jax.ShapeDtypeStruct((LEN, 2), F32),
            jax.ShapeDtypeStruct((1, ql.shape[1]), F32),
            jax.ShapeDtypeStruct((1, ql.shape[1]), F32),
        ],
        grid_spec=pltpu.PrefetchScalarGridSpec(
            num_scalar_prefetch=1,
            grid=(heads,),
            in_specs=[col, col, col, col, pl.BlockSpec((1, LEN, 1), lambda h, p: (h, 0, 0)),
                      col, col, one, one, gain, gain, table, table],
            out_specs=[col, col, col, pl.BlockSpec((LEN, 2), lambda h, p: (0, 0)), gain, gain],
            scratch_shapes=[pltpu.VMEM((LEN, HEAD_DIM), F32)] * 3,
        ),
        cost_estimate=pl.CostEstimate(
            flops=heads * LEN * LEN * HEAD_DIM * 7, bytes_accessed=24 << 20, transcendentals=heads * LEN * LEN
        ),
        name="attend_back",
    )(prefix, qb, kb, vb, dob, lse, ql, kl, sq, sk, gq, gk, cos, sin)


FTILE = 256


def expert_kernel(b, c, wg, wu, wd, gate, hg, dg, du, dgate):
    g = dot(b[...], wg[...])
    u = dot(b[...], wu[...])
    back = dot_nt(c[...], wd[...])
    sigma = jax.nn.sigmoid(g)
    silu = g * sigma
    h = silu * u
    weight = gate[0]
    hg[...] = (weight * h).astype(BF)
    part = jnp.sum(h * back, -1, keepdims=True)
    dh = weight * back
    dg[...] = (dh * u * (sigma * (1.0 + g * (1.0 - sigma)))).astype(BF)
    du[...] = (dh * silu).astype(BF)

    @pl.when(pl.program_id(1) == 0)
    def _():
        dgate[0] = part

    @pl.when(pl.program_id(1) > 0)
    def _():
        dgate[0] += part


def experts(b, c, wg, wu, wd, gate):
    rows, width = b.shape
    count = gate.shape[0]
    ff = wg.shape[1] // count
    tiles = ff // FTILE
    whole = pl.BlockSpec((rows, width), lambda j, f: (0, 0), pipeline_mode=pl.Buffered(1))
    up = pl.BlockSpec((width, FTILE), lambda j, f: (0, j * tiles + f))
    one = pl.BlockSpec((1, rows, 1), lambda j, f: (j, 0, 0))
    out = pl.BlockSpec((rows, FTILE), lambda j, f: (0, j * tiles + f))
    return pl.pallas_call(
        expert_kernel,
        grid=(count, tiles),
        in_specs=[whole, whole, up, up, pl.BlockSpec((FTILE, width), lambda j, f: (f, j)), one],
        out_specs=[out, out, out, one],
        out_shape=[jax.ShapeDtypeStruct((rows, count * ff), BF)] * 3
        + [jax.ShapeDtypeStruct((count, rows, 1), F32)],
        cost_estimate=pl.CostEstimate(
            flops=6 * rows * width * count * ff, bytes_accessed=80 << 20, transcendentals=rows * count * ff
        ),
        name="experts",
    )(b, c, wg, wu, wd, gate)


def down_kernel(hg, wd, out, total):
    j = pl.program_id(0)

    @pl.when(j == 0)
    def _():
        total[...] = dot(hg[...], wd[...])

    @pl.when(j > 0)
    def _():
        total[...] += dot(hg[...], wd[...])

    @pl.when(j == pl.num_programs(0) - 1)
    def _():
        out[...] = total[...]


def down(hg, wd, width):
    rows = hg.shape[0]
    ff = wd.shape[0]
    count = hg.shape[1] // ff
    return pl.pallas_call(
        down_kernel,
        grid=(count,),
        in_specs=[
            pl.BlockSpec((rows, ff), lambda j: (0, j)),
            pl.BlockSpec((ff, width), lambda j: (0, j)),
        ],
        out_specs=pl.BlockSpec((rows, width), lambda j: (0, 0), pipeline_mode=pl.Buffered(1)),
        out_shape=jax.ShapeDtypeStruct((rows, width), F32),
        scratch_shapes=[pltpu.VMEM((rows, width), F32)],
        cost_estimate=pl.CostEstimate(
            flops=2 * rows * width * count * ff, bytes_accessed=40 << 20, transcendentals=0
        ),
        name="down",
    )(hg, wd)


def body(
    tokens,
    routes,
    prefix,
    query_weight,
    key_weight,
    value_weight,
    output_weight,
    router_weight,
    attention_gain,
    feedforward_gain,
    query_gain,
    key_gain,
    expert_in,
    expert_down,
    cotangent,
):
    count = lax.axis_size("expert")
    here = lax.axis_index("expert")
    group_here = lax.axis_index("group")
    rows, width = tokens.shape
    cols = width // count
    experts_all = router_weight.shape[1]
    local = expert_in.shape[1]
    ff_rows = expert_down.shape[0]
    ff = expert_in.shape[2] // 2
    master = query_weight.shape[0]

    def gather(value):
        return lax.all_gather(value, "group", axis=0, tiled=True)

    def scatter(value):
        return lax.psum_scatter(value, "group", scatter_dimension=0, tiled=True)

    def own_cols(weight):
        return lax.dynamic_slice(weight, (0, here * cols), (master, cols)).astype(BF)

    small = jnp.concatenate(
        [
            jnp.stack([attention_gain, feedforward_gain, query_gain, key_gain]),
            jnp.zeros((4, master), F32),
            router_weight.T,
        ]
    ).astype(BF)
    small = lax.all_gather(small, "group", axis=1, tiled=True).astype(F32)
    gain_one, gain_two = small[0:1], small[1:2]
    gain_query = lax.dynamic_slice(small[2:3], (0, here * cols), (1, cols))
    gain_key = lax.dynamic_slice(small[3:4], (0, here * cols), (1, cols))
    router = small[8:].astype(BF)
    qkv_weight = gather(
        jnp.concatenate([own_cols(query_weight), own_cols(key_weight), own_cols(value_weight)], 1)
    )
    out_weight = gather(output_weight.astype(BF))
    gate_weight = gather(expert_in[:, :, :ff].astype(BF).reshape(master, local * ff))
    up_weight = gather(expert_in[:, :, ff:].astype(BF).reshape(master, local * ff))
    down_weight = gather(expert_down.astype(BF).reshape(ff_rows, local * width))

    expert_ids = jnp.arange(experts_all, dtype=jnp.int32)
    selected = jnp.sum((routes[:, :, None] == expert_ids).astype(F32), 1)
    sent = jnp.concatenate(
        [tokens, jnp.pad(selected, ((0, 0), (0, 128 - experts_all))).astype(BF)], 1
    )
    sent = ring_gather(sent, count, here)
    x_all = sent[:, :width].astype(F32)
    chosen = sent[:, width : width + experts_all].astype(F32)

    steps = jnp.arange(HEAD_DIM // 2).astype(F32)
    freq = jnp.exp(steps * (-2.0 * math.log(THETA) / HEAD_DIM))
    angle = jnp.arange(LEN).astype(F32)[:, None] * freq[None, :]
    cosine = jnp.concatenate([jnp.cos(angle)] * 2, 1)
    sine = jnp.concatenate([-jnp.sin(angle), jnp.sin(angle)], 1)

    hidden_one = (x_all * row_scale(x_all) * gain_one).astype(BF)
    qkv = dot(hidden_one, qkv_weight)
    query_lin, key_lin = qkv[:, :cols], qkv[:, cols : 2 * cols]
    value_bf = qkv[:, 2 * cols :].astype(BF)
    squares = jnp.stack([jnp.sum(query_lin * query_lin, -1), jnp.sum(key_lin * key_lin, -1)])
    scales = lax.rsqrt(exchange_sum(squares, count) / width + EPS)
    scale_query, scale_key = scales[0][:, None], scales[1][:, None]
    attended, query_bf, key_bf, lse = attend(
        prefix, query_lin, key_lin, value_bf, scale_query, scale_key, gain_query, gain_key, cosine, sine
    )
    attended_bf = jnp.zeros((rows, width), BF)
    for step in range(count):
        block = lax.dynamic_slice(attended, (((here + step) % count) * rows, 0), (rows, cols))
        if step:
            block = shift(block, count, step)
        attended_bf = lax.dynamic_update_slice(attended_bf, block, (0, ((here - step) % count) * cols))

    cot, attended_bf = lax.optimization_barrier((cotangent, attended_bf))
    cot_all = ring_gather(cot, count, here)

    xfloat = tokens.astype(F32)
    resid = xfloat + dot(attended_bf, out_weight)
    scale_two = row_scale(resid)
    normed_two = resid * scale_two
    hidden_two = (normed_two * gain_two).astype(BF)
    b_all = ring_gather(hidden_two, count, here)
    probs = jax.nn.softmax(dot_nt(b_all, router), -1)
    gates = lax.dynamic_slice(probs * chosen, (0, here * local), (LEN, local))
    hg, dg, du, dgate = experts(b_all, cot_all, gate_weight, up_weight, down_weight, gates.T[:, :, None])

    dgate = dgate[:, :, 0].T * lax.dynamic_slice(chosen, (0, here * local), (LEN, local))
    dprobs = lax.dynamic_update_slice(jnp.zeros((LEN, 128), F32), dgate, (0, here * local))
    grad_down = jnp.einsum(
        "tjf,td->fjd", hg.reshape(LEN, local, ff), cot_all, preferred_element_type=F32
    ).astype(BF).reshape(ff, local * width)
    grad_down = scatter(grad_down).astype(F32).reshape(ff_rows, local, width)

    def back_term(block):
        at = block * rows
        left = lax.dynamic_slice(dg, (at, 0), (rows, local * ff))
        right = lax.dynamic_slice(du, (at, 0), (rows, local * ff))
        return jnp.concatenate(
            [
                dot_nt(left, gate_weight) + dot_nt(right, up_weight),
                lax.dynamic_slice(dprobs, (at, 0), (rows, 128)),
            ],
            1,
        )

    back = ring_scatter(back_term, count, here)
    grad_gate = scatter(dot_tn(b_all, dg).astype(BF))
    grad_up = scatter(dot_tn(b_all, du).astype(BF))
    grad_in = jnp.concatenate(
        [grad_gate.reshape(master, local, ff), grad_up.reshape(master, local, ff)], 2
    ).astype(F32)

    own_probs = jax.nn.softmax(dot_nt(hidden_two, router), -1)
    grad_probs = back[:, width : width + experts_all]
    grad_logits = (
        own_probs * (grad_probs - jnp.sum(grad_probs * own_probs, -1, keepdims=True))
    ).astype(BF)
    grad_router = dot_tn(grad_logits, hidden_two)
    grad_two = back[:, :width] + dot(grad_logits, router)
    gain_two_term = jnp.sum(grad_two * normed_two, 0)
    grad_out = cotangent.astype(F32)
    grad_resid = grad_out + norm_back(resid, scale_two, grad_two * gain_two)
    grad_attn_out = grad_resid.astype(BF)
    grad_attended = dot_nt(grad_attn_out, out_weight).astype(BF)
    heads_grad = jnp.zeros((LEN, cols), BF)
    for step in range(count):
        block = lax.dynamic_slice(grad_attended, (0, ((here + step) % count) * cols), (rows, cols))
        if step:
            block = shift(block, count, step)
        heads_grad = lax.dynamic_update_slice(heads_grad, block, (((here - step) % count) * rows, 0))
    grad_out_weight = scatter(dot_tn(attended_bf, grad_attn_out).astype(BF))

    wq, wk, dvl, inner, gain_q_term, gain_k_term = attend_back(
        prefix, query_bf, key_bf, value_bf, heads_grad, lse, query_lin, key_lin,
        scale_query, scale_key, gain_query, gain_key, cosine, sine,
    )
    inner = exchange_sum(inner.T, count) / width
    dql = scale_query * wq - query_lin * (scale_query**3 * inner[0][:, None])
    dkl = scale_key * wk - key_lin * (scale_key**3 * inner[1][:, None])
    dqkv = jnp.concatenate([dql.astype(BF), dkl.astype(BF), dvl], 1)

    def token_term(block):
        return dot_nt(lax.dynamic_slice(dqkv, (block * rows, 0), (rows, 3 * cols)), qkv_weight)

    grad_hidden = ring_scatter(token_term, count, here)
    grad_qkv = scatter(dot_tn(hidden_one, dqkv).astype(BF))

    partial, grad_hidden = lax.optimization_barrier((down(hg, down_weight, width), grad_hidden))

    def down_term(block):
        return lax.dynamic_slice(partial, (block * rows, 0), (rows, width))

    output = (resid + ring_scatter(down_term, count, here)).astype(BF)

    scale_one = row_scale(xfloat)
    gain_one_term = jnp.sum(grad_hidden * (xfloat * scale_one), 0)
    grad_tokens = grad_resid + norm_back(xfloat, scale_one, grad_hidden * gain_one)

    def own_part(value):
        return lax.dynamic_slice(value, (0, group_here * master), (value.shape[0], master))

    def spread(value):
        return lax.dynamic_update_slice(jnp.zeros((1, width), F32), value, (0, here * cols))

    sums = jnp.concatenate(
        [
            gain_one_term[None],
            gain_two_term[None],
            spread(gain_q_term),
            spread(gain_k_term),
            jnp.zeros((4, width), F32),
            grad_router,
        ]
    )
    sums = own_part(lax.psum(sums, ("group", "expert")))
    grad_out_weight = lax.psum(grad_out_weight, "expert").astype(F32)
    grad_qkv = lax.all_gather(grad_qkv, "expert", axis=0, tiled=False)
    grad_q, grad_k, grad_v = [
        grad_qkv[:, :, i * cols : (i + 1) * cols].transpose(1, 0, 2).reshape(master, width).astype(F32)
        for i in range(3)
    ]
    return (
        output,
        grad_tokens,
        grad_q,
        grad_k,
        grad_v,
        grad_out_weight,
        sums[8:].T,
        sums[0],
        sums[1],
        sums[2],
        sums[3],
        grad_in,
        grad_down,
    )


def solution(mesh):
    in_specs = (
        P(("group", "expert"), None),
        P(("group", "expert"), None),
        P("group"),
        P("group", None),
        P("group", None),
        P("group", None),
        P("group", None),
        P("group", None),
        P("group"),
        P("group"),
        P("group"),
        P("group"),
        P("group", "expert", None),
        P("group", "expert", None),
        P(("group", "expert"), None),
    )
    out_specs = (
        P(("group", "expert"), None),
        P(("group", "expert"), None),
        P("group", None),
        P("group", None),
        P("group", None),
        P("group", None),
        P("group", None),
        P("group"),
        P("group"),
        P("group"),
        P("group"),
        P("group", "expert", None),
        P("group", "expert", None),
    )
    return jax.shard_map(body, mesh=mesh, in_specs=in_specs, out_specs=out_specs, check_vma=False)
```

```python
import functools
import math

import jax
import jax.numpy as jnp
from jax import lax
from jax.experimental import pallas as pl
from jax.experimental.pallas import tpu as pltpu
from jax.sharding import PartitionSpec as P

HEADS = 16
HEAD_DIM = 128
LEN = 1024
MAX_PREFIX = LEN // 2
QBLOCK = 256
EPS = 1e-05
THETA = 10000.0
BF = jnp.bfloat16
F32 = jnp.float32
MESH = pl.DeviceIdType.MESH
LANES = 128
SHORT = pl.CostEstimate(flops=1000000, bytes_accessed=1000000, transcendentals=0)


def dot(left, right):
    return jnp.dot(left, right, preferred_element_type=F32)


def dot_nt(left, right):
    return lax.dot_general(left, right, (((1,), (1,)), ((), ())), preferred_element_type=F32)


def dot_tn(left, right):
    return lax.dot_general(left, right, (((0,), (0,)), ((), ())), preferred_element_type=F32)


def row_scale(values):
    return lax.rsqrt(jnp.mean(values * values, -1, keepdims=True) + EPS)


def norm_back(values, scale_rows, upstream):
    inner = jnp.mean(upstream * values, -1, keepdims=True)
    return scale_rows * upstream - values * (scale_rows * scale_rows * scale_rows) * inner


def shift(value, count, step):
    return lax.ppermute(value, "expert", [(i, (i + step) % count) for i in range(count)])


class Ring:
    def __init__(self, value, arrived, count, here):
        self.value, self.count, self.here = value, count, here
        self.step = 1
        self.total = self.term() + arrived.astype(F32)

    def term(self):
        rows = self.value.shape[0] // self.count
        block = (self.here - 1 - self.step) % self.count
        return lax.dynamic_slice(self.value, (block * rows, 0), (rows, self.value.shape[1]))

    def hop(self, *done):
        arrived = shift(self.total.astype(BF), self.count, 1)
        self.step += 1
        self.total = self.term() + after(arrived, *done).astype(F32)
        return self.total

    def finish(self, *done):
        while self.step < self.count - 1:
            self.hop(*done)
        return self.total


def exchange_kernel(count, value, out, slots, send_sem, recv_sem):
    here = lax.axis_index("expert")
    others = [lax.rem(here + step, count) for step in range(1, count)]
    barrier = pltpu.get_barrier_semaphore()
    for other in others:
        pl.semaphore_signal(barrier, inc=1, device_id={"expert": other}, device_id_type=MESH)
    pl.semaphore_wait(barrier, count - 1)
    copies = [
        pltpu.make_async_remote_copy(
            src_ref=value,
            dst_ref=slots.at[i],
            send_sem=send_sem.at[i],
            recv_sem=recv_sem.at[i],
            device_id={"expert": other},
            device_id_type=MESH,
        )
        for i, other in enumerate(others)
    ]
    for copy in copies:
        copy.start()
    for copy in copies:
        copy.wait()
    total = value[...]
    for i in range(count - 1):
        total = total + slots[i]
    out[...] = total


def exchange_sum(value, count, call):
    return pl.pallas_call(
        functools.partial(exchange_kernel, count),
        out_shape=jax.ShapeDtypeStruct(value.shape, F32),
        in_specs=[pl.BlockSpec(memory_space=pltpu.VMEM)],
        out_specs=pl.BlockSpec(memory_space=pltpu.VMEM),
        scratch_shapes=[
            pltpu.VMEM((count - 1,) + value.shape, F32),
            pltpu.SemaphoreType.DMA((count - 1,)),
            pltpu.SemaphoreType.DMA((count - 1,)),
        ],
        compiler_params=pltpu.CompilerParams(collective_id=call, has_side_effects=True),
        name="exchange%d" % call,
    )(value)


def after(value, *done):
    return lax.optimization_barrier((value,) + done)[0]


PIECES = 2


def gather_kernel(count, arrays, *refs):
    values, wholes = refs[:arrays], refs[arrays : 2 * arrays]
    local, sems = refs[2 * arrays : 3 * arrays], refs[3 * arrays :]
    send_sem, recv_sem, in_sem, out_sem = sems
    here = lax.axis_index("expert")
    right, left = lax.rem(here + 1, count), lax.rem(here + count - 1, count)
    other_core = flipped(lax.axis_index("group"), 1)

    def hop(array, step, piece):
        rows = values[array].shape[0]
        size = rows // PIECES
        owner = lax.rem(here - step + count, count)
        place = wholes[array].at[pl.ds(pl.multiple_of(owner * rows + piece * size, size), size)]
        return pltpu.make_async_remote_copy(
            src_ref=place if step else values[array].at[pl.ds(piece * size, size)],
            dst_ref=place,
            send_sem=send_sem.at[array, step, piece],
            recv_sem=recv_sem.at[array, step, piece],
            device_id={"expert": right},
            device_id_type=MESH,
        )

    loads = [pltpu.make_async_copy(values[i], local[i], in_sem.at[i]) for i in range(arrays)]

    @pl.when(pl.program_id(0) == 0)
    def _():
        barrier = pltpu.get_barrier_semaphore()
        for other in (left, right):
            pl.semaphore_signal(barrier, inc=1, device_id={"expert": other}, device_id_type=MESH)
        pl.semaphore_signal(barrier, inc=1, device_id={"group": other_core}, device_id_type=MESH)
        pl.semaphore_wait(barrier, 3)
        for i in range(arrays):
            for piece in range(PIECES):
                hop(i, 0, piece).start()
            loads[i].start()

    def rest():
        stores = []
        for i in range(arrays):
            rows = values[i].shape[0]
            loads[i].wait()
            stores.append(
                pltpu.make_async_copy(
                    local[i], wholes[i].at[pl.ds(pl.multiple_of(here * rows, rows), rows)], out_sem.at[i]
                )
            )
            stores[i].start()
        for i in range(arrays):
            for step in range(1, count - 1):
                for piece in range(PIECES):
                    hop(i, step - 1, piece).wait_recv()
                    hop(i, step, piece).start()
        for i in range(arrays):
            stores[i].wait()
            for piece in range(PIECES):
                hop(i, count - 2, piece).wait_recv()
                for step in range(count - 1):
                    hop(i, step, piece).wait_send()

    return rest


def gather_only(count, arrays, *refs):
    gather_kernel(count, arrays, *refs)()


def gather_scratch(values, count):
    arrays = len(values)
    hops = pltpu.SemaphoreType.DMA((arrays, count - 1, PIECES))
    return [pltpu.VMEM(v.shape, v.dtype) for v in values] + [
        hops, hops, pltpu.SemaphoreType.DMA((arrays,)), pltpu.SemaphoreType.DMA((arrays,))
    ]


def gather_rows(values, count, call):
    arrays = len(values)
    return pl.pallas_call(
        functools.partial(gather_only, count, arrays),
        grid=(1,),
        out_shape=[jax.ShapeDtypeStruct((count * v.shape[0],) + v.shape[1:], v.dtype) for v in values],
        in_specs=[pl.BlockSpec(memory_space=pl.ANY)] * arrays,
        out_specs=[pl.BlockSpec(memory_space=pl.ANY)] * arrays,
        scratch_shapes=gather_scratch(values, count),
        compiler_params=pltpu.CompilerParams(collective_id=call, has_side_effects=True),
        cost_estimate=SHORT,
        name="gather%d" % call,
    )(*values)


PREP_ROWS = 32


def prep_kernel(count, halves, value, up, lower, whole, out1, out2, *scratch):
    rest = gather_kernel(count, 1, value, whole, *scratch)
    ff = up.shape[2] // 2
    for pair, out in enumerate((out1, out2)):
        for j in range(PAIR):
            row = up[:, pair * PAIR + j, :].astype(BF)
            out[:, j * ff : (j + 1) * ff] = row[:, :ff]
            out[:, (PAIR + j) * ff : (PAIR + j + 1) * ff] = row[:, ff:]

        for j in range(PAIR):

            @pl.when(pl.program_id(0) // halves == j)
            def _():
                out[:, 2 * PAIR * ff :] = lower[:, pair * PAIR + j, :].astype(BF)

    pl.when(pl.program_id(0) == pl.num_programs(0) - 1)(rest)


def gather_and_prep(value, expert_in, expert_down, count, call):
    master, local, both = expert_in.shape
    halves = expert_down.shape[0] // PREP_ROWS
    width = expert_down.shape[2]
    columns = PAIR * both + width
    anywhere = pl.BlockSpec(memory_space=pl.ANY)
    return pl.pallas_call(
        functools.partial(prep_kernel, count, halves),
        grid=(master // PREP_ROWS,),
        in_specs=[
            anywhere,
            pl.BlockSpec((PREP_ROWS, local, both), lambda i: (i, 0, 0)),
            pl.BlockSpec((PREP_ROWS, local, width), lambda i: (lax.rem(i, halves), 0, 0)),
        ],
        out_specs=[anywhere] + [pl.BlockSpec((PREP_ROWS, columns), lambda i: (i, 0))] * 2,
        out_shape=[jax.ShapeDtypeStruct((count * value.shape[0],) + value.shape[1:], value.dtype)]
        + [jax.ShapeDtypeStruct((master, columns), BF)] * 2,
        scratch_shapes=gather_scratch((value,), count),
        compiler_params=pltpu.CompilerParams(collective_id=call, has_side_effects=True),
        cost_estimate=SHORT,
        name="gather%d" % call,
    )(value, expert_in, expert_down)


SLOTS = 3


def grads_kernel(count, hg, b, cot, dg, du, *refs):
    if count:
        partial, grad, *refs = refs
        weights, (out, first_in, heads_out), refs = refs[:count], refs[count : count + 3], refs[count + 3 :]
    else:
        out, *refs = refs
    hg_held, b_held, cot_held, dg_held, du_held, sent, landed, sem, send_sem, recv_sem = refs[:10]
    step = pl.program_id(0)
    group = lax.axis_index("group")
    core = lax.rem(group, 2)
    other = flipped(group, 1)
    size, columns = out.shape[0], cot_held.shape[1]
    chips = landed.shape[0]
    loads = [
        pltpu.make_async_copy(source, held, sem.at[i])
        for i, (source, held) in enumerate(
            ((hg, hg_held), (cot, cot_held), (b, b_held), (dg, dg_held), (du, du_held))
        )
    ]

    def copy(chip):
        return pltpu.make_async_remote_copy(
            src_ref=sent.at[lax.rem(chip, SLOTS)], dst_ref=landed.at[chip], send_sem=send_sem.at[chip], recv_sem=recv_sem.at[chip],
            device_id={"group": other}, device_id_type=MESH,
        )

    def terms(place):
        left_down = jnp.concatenate([hg_held[place, j] for j in range(PAIR)], -1)
        left = b_held[:, pl.ds(pl.multiple_of(place * size, size), size)]
        return (left_down, cot_held), (left, dg_held), (left, du_held)

    lanes = [slice(i * columns, (i + 1) * columns) for i in range(3)]
    if count:
        here = lax.axis_index("expert")
        right, left = lax.rem(here + 1, count), lax.rem(here + count - 1, count)
        rows = partial.shape[0] // count
        first = pltpu.make_async_remote_copy(
            src_ref=partial.at[pl.ds(pl.multiple_of(left * rows, rows), rows)], dst_ref=first_in,
            send_sem=refs[10].at[0], recv_sem=refs[10].at[1], device_id={"expert": right}, device_id_type=MESH,
        )
        heads_sent, heads_send, heads_recv, own_sem = refs[11:]
        own_rows, cols = grad.shape[0], heads_out.shape[1]
        others = [lax.rem(here + number, count) for number in range(1, count)]
        own_place = heads_out.at[pl.ds(pl.multiple_of(here * own_rows, own_rows), own_rows)]

        def heads(other):
            at = pl.ds(pl.multiple_of(other * cols, cols), cols)
            total = None
            for i, weight in enumerate(weights):
                term = dot_nt(grad[:, i * cols : (i + 1) * cols], weight[at, :])
                total = term if total is None else total + term
            return total.astype(BF)

        heads_copies = [
            pltpu.make_async_remote_copy(
                src_ref=heads_sent.at[i], dst_ref=own_place, send_sem=heads_send.at[i], recv_sem=heads_recv.at[i],
                device_id={"expert": device}, device_id_type=MESH,
            )
            for i, device in enumerate(others)
        ]

    @pl.when(step == 0)
    def _():
        barrier = pltpu.get_barrier_semaphore()
        pl.semaphore_signal(barrier, inc=1, device_id={"group": other}, device_id_type=MESH)
        if count:
            for device in others:
                pl.semaphore_signal(barrier, inc=1, device_id={"expert": device}, device_id_type=MESH)
        for load in loads:
            load.start()
        pl.semaphore_wait(barrier, count if count else 1)
        if count:
            for i, device in enumerate(others):
                heads_sent[i] = heads(device)
                heads_copies[i].start()
            first.start()
            heads_sent[count - 1] = heads(here)
            own_copy = pltpu.make_async_copy(heads_sent.at[count - 1], own_place, own_sem)
            own_copy.start()
        loads[0].wait()
        loads[2].wait()
        for i, (left_value, right_ref) in enumerate(terms(1 - core)):
            loads[(1, 3, 4)[i]].wait()
            sent[0, :, lanes[i]] = dot_tn(left_value, right_ref[...]).astype(BF)
        copy(0).start()

    @pl.when((step > 0) & (step < chips))
    def _():
        @pl.when(step >= SLOTS)
        def _():
            copy(step - SLOTS).wait_send()

        slot = lax.rem(step, SLOTS)
        for i, (left_value, right_ref) in enumerate(terms(2 * step + 1 - core)):
            sent[slot, :, lanes[i]] = dot_tn(left_value, right_ref[...]).astype(BF)
        copy(step).start()

    @pl.when(step >= chips)
    def _():
        chip = step - chips
        copy(chip).wait_recv()
        for i, (left_value, right_ref) in enumerate(terms(2 * chip + core)):
            total = dot_tn(left_value, right_ref[...]) + landed[chip, :, lanes[i]].astype(F32)
            out[:, lanes[i]] = total.astype(BF)

    @pl.when(step == 2 * chips - 1)
    def _():
        for chip in range(max(chips - SLOTS, 0), chips):
            copy(chip).wait_send()
        if count:
            pltpu.make_async_copy(heads_sent.at[count - 1], own_place, own_sem).wait()
            for copied in heads_copies:
                copied.wait()
            first.wait()


def grad_terms(hg, b, cot, dg, du, call, partial=None, grad=None, dense=None, count=0):
    blocks, _, rows, block = hg.shape
    size = b.shape[1] // blocks
    columns = cot.shape[1]
    chips = blocks // 2
    anywhere = pl.BlockSpec(memory_space=pl.ANY)
    dma = pltpu.SemaphoreType.DMA
    operands, in_specs = [hg, b, cot, dg, du], [anywhere] * 5
    out_specs = [pl.BlockSpec((size, 3 * columns), lambda p: (jnp.maximum(p - chips, 0), 0))]
    out_shape = [jax.ShapeDtypeStruct((chips * size, 3 * columns), BF)]
    scratch = (
        [pltpu.VMEM(hg.shape, BF)]
        + [pltpu.VMEM((rows, columns), BF)] * 4
        + [pltpu.VMEM((min(chips, SLOTS), size, 3 * columns), BF), pltpu.VMEM((chips, size, 3 * columns), BF)]
        + [dma((5,)), dma((chips,)), dma((chips,))]
    )
    if count:
        own_rows, cols = rows // count, columns // count
        once = pl.Buffered(1)
        operands += [partial, grad] + [dense] * count
        in_specs += [anywhere, pl.BlockSpec(grad.shape, lambda p: (0, 0), pipeline_mode=once)]
        in_specs += [pl.BlockSpec((columns, cols), lambda p, j=j: (0, 3 + j), pipeline_mode=once) for j in range(count)]
        out_specs += [anywhere, anywhere]
        out_shape += [jax.ShapeDtypeStruct((own_rows, columns), BF), jax.ShapeDtypeStruct((rows, cols), BF)]
        scratch += [dma((2,)), pltpu.VMEM((count, own_rows, cols), BF), dma((count - 1,)), dma((count - 1,)), dma]
    return pl.pallas_call(
        functools.partial(grads_kernel, count),
        grid=(blocks,),
        in_specs=in_specs,
        out_specs=out_specs,
        out_shape=out_shape,
        scratch_shapes=scratch,
        compiler_params=pltpu.CompilerParams(
            collective_id=call, has_side_effects=True, vmem_limit_bytes=67043328
        ),
        cost_estimate=SHORT,
        name="grads%d" % call,
    )(*operands)


def heads_kernel(count, value, out, send_sem, recv_sem, own_sem):
    here = lax.axis_index("expert")
    rows, cols = out.shape[0], value.shape[1]
    others = [lax.rem(here + step, count) for step in range(1, count)]
    barrier = pltpu.get_barrier_semaphore()
    for other in others:
        pl.semaphore_signal(barrier, inc=1, device_id={"expert": other}, device_id_type=MESH)
    pl.semaphore_wait(barrier, count - 1)
    place = out.at[:, pl.ds(pl.multiple_of(here * cols, cols), cols)]

    def block(other):
        return value.at[pl.ds(pl.multiple_of(other * rows, rows), rows)]

    copies = [
        pltpu.make_async_remote_copy(
            src_ref=block(other), dst_ref=place, send_sem=send_sem.at[i], recv_sem=recv_sem.at[i],
            device_id={"expert": other}, device_id_type=MESH,
        )
        for i, other in enumerate(others)
    ]
    for copy in copies:
        copy.start()
    own = pltpu.make_async_copy(block(here), place, own_sem)
    own.start()
    own.wait()
    for copy in copies:
        copy.wait()


def heads_to_rows(value, count, call):
    vmem = pl.BlockSpec(memory_space=pltpu.VMEM)
    dma = pltpu.SemaphoreType.DMA
    return pl.pallas_call(
        functools.partial(heads_kernel, count),
        out_shape=jax.ShapeDtypeStruct((value.shape[0] // count, value.shape[1] * count), value.dtype),
        in_specs=[vmem],
        out_specs=vmem,
        scratch_shapes=[dma((count - 1,)), dma((count - 1,)), dma],
        compiler_params=pltpu.CompilerParams(collective_id=call, has_side_effects=True),
        cost_estimate=SHORT,
        name="heads%d" % call,
    )(value)


def flipped(index, mask):
    bit = 1
    while bit <= mask:
        if mask & bit:
            index = index + bit * (1 - 2 * lax.rem(lax.div(index, bit), 2))
        bit *= 2
    return index


def subsets(bits):
    sums = [0]
    for bit in bits:
        sums = sums + [value + bit for value in sums]
    return sums


def tail_kernel(
    count, groups, grads, weight, hidden, output_sum, normed, sums, rows_out, *refs
):
    final_outs, sums_out, refs = refs[:4], refs[4], refs[5:]
    (
        query_out, key_out, value_out, output_out, final_sem,
        sent, landed, core_out, core_in, held, step_in, done, part_sent, part_in, small, small_in, small_sum,
        all_in, own_sem, token_send, token_recv, core_send, core_recv, step_send, step_recv, whole_send,
        whole_recv, part_send, part_recv, sum_send, sum_recv, small_send, small_recv, all_send, all_recv,
    ) = refs
    here, group = lax.axis_index("expert"), lax.axis_index("group")
    right, left = lax.rem(here + 1, count), lax.rem(here + count - 1, count)
    others = [lax.rem(here + step, count) for step in range(1, count)]
    bits = [1 << i for i in range(1, groups.bit_length() - 1)]
    orders = (bits, bits[::-1])
    barrier = pltpu.get_barrier_semaphore()
    for other in others:
        pl.semaphore_signal(barrier, inc=1, device_id={"expert": other}, device_id_type=MESH)
    peers = [lax.rem(group + step, groups) for step in range(1, groups)]
    for peer in peers:
        pl.semaphore_signal(barrier, inc=1, device_id={"group": peer}, device_id_type=MESH)
    pl.semaphore_wait(barrier, count + groups - 2)

    rows, width = rows_out.shape
    half = width // 2
    master, columns = held.shape[1:]
    cols = width // count
    slab = master // count

    def to(axis, other, source, target, send, receive):
        return pltpu.make_async_remote_copy(
            src_ref=source, dst_ref=target, send_sem=send, recv_sem=receive,
            device_id={axis: other}, device_id_type=MESH,
        )

    rest = subsets(bits)

    core = [
        to("group", flipped(group, 1), core_out.at[i], core_in.at[i], core_send.at[i], core_recv.at[i])
        for i in range(len(rest))
    ]
    backward = list(enumerate(rest))[::-1]

    def own_term(block):
        lanes = pl.ds(pl.multiple_of(block * master, master), master)
        return dot_tn(hidden[:, lanes], grads[...])

    def token_block(step, piece):
        block = lax.rem(here - 1 - step + count, count)
        return dot_nt(grads[pl.ds(pl.multiple_of(block * rows, rows), rows), :],
                      weight[piece * half : (piece + 1) * half, :])

    def token_hop(step, piece):
        return to("expert", right, sent.at[step % 2, piece], landed.at[step, piece],
                  token_send.at[step, piece], token_recv.at[step, piece])

    for piece in range(2):
        sent[0, piece] = token_block(0, piece).astype(BF)
        token_hop(0, piece).start()

    def token_step(step):
        terms = [token_block(step, piece) for piece in range(2)]
        for piece in range(2):
            token_hop(step - 1, piece).wait_recv()
            total = terms[piece] + landed[step - 1, piece].astype(F32)
            if step < count - 1:
                if step >= 2:
                    token_hop(step - 2, piece).wait_send()
                sent[step % 2, piece] = total.astype(BF)
                token_hop(step, piece).start()
            else:
                rows_out[:, piece * half : (piece + 1) * half] = total

    def moves(order, level):
        bit = order[level]
        sends = [r for r in rest if r & bit and not r & sum(order[:level])]
        return bit, sends, sum(len(rest) >> (i + 1) for i in range(level))

    outs = (query_out, key_out, value_out)
    pieces = len(outs)

    def whole_hop(step, piece):
        owner = lax.rem(here - step + count, count)
        target = outs[piece].at[:, pl.ds(pl.multiple_of(owner * cols, cols), cols)]
        source = done.at[:, pl.ds(piece * cols, cols)] if step == 0 else target
        return to("expert", right, source, target, whole_send.at[step, piece], whole_recv.at[step, piece])

    own = [
        pltpu.make_async_copy(
            done.at[:, pl.ds(piece * cols, cols)],
            outs[piece].at[:, pl.ds(pl.multiple_of(here * cols, cols), cols)],
            own_sem.at[piece],
        )
        for piece in range(pieces)
    ]

    def whole_start():
        for piece in range(pieces):
            whole_hop(0, piece).start()
        for copy in own:
            copy.start()

    streams = [(slice(0, columns // 2), orders[0]), (slice(columns // 2, columns), orders[1])]

    def step_copies(stream, level):
        lanes, order = streams[stream]
        bit, sends, first = moves(order, level)
        return [
            to("group", flipped(group, bit), held.at[rest.index(r), :, lanes],
               step_in.at[stream, first + i],
               step_send.at[stream, first + i], step_recv.at[stream, first + i])
            for i, r in enumerate(sends)
        ]

    copies = [[step_copies(stream, level) for level in range(len(bits))] for stream in range(2)]
    for i, r in backward:
        core_out[i] = own_term(flipped(group, 1 + r)).astype(BF)
        core[i].start()
    for i, r in backward:
        term = own_term(flipped(group, r))
        core[i].wait_recv()
        held[i] = (term + core_in[i].astype(F32)).astype(BF)
        for stream in range(2):
            sends = moves(streams[stream][1], 0)[1]
            if r in sends:
                copies[stream][0][sends.index(r)].start()

    def reduce_step(level):
        for stream in range(2):
            lanes, order = streams[stream]
            bit, sends, first = moves(order, level)
            for i, r in enumerate(sends):
                copies[stream][level][i].wait()
                kept = rest.index(r - bit)
                total = (held[kept, :, lanes].astype(F32) + step_in[stream, first + i].astype(F32)).astype(BF)
                if level < len(bits) - 1:
                    held[kept, :, lanes] = total
                else:
                    done[:, lanes] = total
            if level < len(bits) - 1:
                for copy in copies[stream][level + 1]:
                    copy.start()

    def slab_of(other):
        return pl.ds(pl.multiple_of(other * slab, slab), slab)

    def slab_hop(step):
        return to("expert", right, part_sent.at[step], part_in.at[step], part_send.at[step], part_recv.at[step])

    def slab_step(step):
        total = output_sum[slab_of(lax.rem(here - 1 - step + count, count)), :].astype(F32)
        if step:
            slab_hop(step - 1).wait_recv()
            total = total + part_in[step - 1].astype(F32)
        if step < count - 1:
            part_sent[step] = total.astype(BF)
            slab_hop(step).start()
        else:
            output_out[slab_of(here), :] = total.astype(BF)

    def sum_hop(step):
        place = output_out.at[slab_of(lax.rem(here - step + count, count))]
        return to("expert", right, place, place, sum_send.at[step], sum_recv.at[step])

    slab_step(0)
    levels = iter(range(len(bits)))
    for step in range(1, count):
        token_step(step)
        slab_step(step)
        level = next(levels, None)
        if level is not None:
            reduce_step(level)
    for level in levels:
        reduce_step(level)
    whole_start()
    sum_hop(0).start()
    small[...] = sums[...]
    small[0:1, :] = jnp.sum(rows_out[...] * normed[...], 0, keepdims=True)
    small_copies = [
        to("group", peer, small.at[:, pl.ds(pl.multiple_of(peer * master, master), master)], small_in.at[i],
           small_send.at[i], small_recv.at[i])
        for i, peer in enumerate(peers)
    ]
    for copy in small_copies:
        copy.start()
    total = small[:, pl.ds(pl.multiple_of(group * master, master), master)]
    for i, copy in enumerate(small_copies):
        copy.wait()
        total = total + small_in[i]
    small_sum[...] = total
    all_copies = [
        to("expert", other, small_sum, all_in.at[i], all_send.at[i], all_recv.at[i]) for i, other in enumerate(others)
    ]
    for copy in all_copies:
        copy.start()
    for step in range(1, count - 1):
        for piece in range(pieces):
            whole_hop(step - 1, piece).wait_recv()
            whole_hop(step, piece).start()
        sum_hop(step - 1).wait_recv()
        sum_hop(step).start()
    for i, copy in enumerate(all_copies):
        copy.wait()
        total = total + all_in[i]
    sums_out[...] = total
    for piece in range(pieces):
        own[piece].wait()
        whole_hop(count - 2, piece).wait_recv()
    sum_hop(count - 2).wait_recv()
    finals = [
        pltpu.make_async_copy(source, target, final_sem.at[i])
        for i, (source, target) in enumerate(zip((query_out, key_out, value_out, output_out), final_outs))
    ]
    for copy in finals:
        copy.start()
    for copy in core:
        copy.wait_send()
    for step in range(count - 1):
        slab_hop(step).wait_send()
        sum_hop(step).wait_send()
        if step >= count - 3:
            for piece in range(2):
                token_hop(step, piece).wait_send()
        for piece in range(pieces):
            whole_hop(step, piece).wait_send()
    for copy in finals:
        copy.wait()


def tail(grads, dense, hidden, output_sum, normed, sums, count, groups, call):
    rows, width = hidden.shape[0] // count, hidden.shape[1]
    own_columns = grads.shape[1]
    master = width // groups
    rest = groups // 2
    slab = master // count
    dma = pltpu.SemaphoreType.DMA
    vmem = pl.BlockSpec(memory_space=pltpu.VMEM)
    return pl.pallas_call(
        functools.partial(tail_kernel, count, groups),
        out_shape=[jax.ShapeDtypeStruct((rows, width), F32)] + [jax.ShapeDtypeStruct((master, width), BF)] * 4
        + [jax.ShapeDtypeStruct((sums.shape[0], master), F32)],
        grid=(1,),
        in_specs=[
            pl.BlockSpec(grads.shape, lambda i: (0, 0)),
            pl.BlockSpec((width, own_columns), lambda i: (0, 0)),
            pl.BlockSpec(hidden.shape, lambda i: (0, 0)),
            pl.BlockSpec(output_sum.shape, lambda i: (0, 0)),
            pl.BlockSpec(normed.shape, lambda i: (0, 0)),
            pl.BlockSpec(sums.shape, lambda i: (0, 0)),
        ],
        out_specs=[vmem] + [pl.BlockSpec(memory_space=pl.ANY)] * 4 + [vmem],
        scratch_shapes=[pltpu.VMEM((master, width), BF)] * 4
        + [
            dma((4,)),
            pltpu.VMEM((2, 2, rows, width // 2), BF),
            pltpu.VMEM((count - 1, 2, rows, width // 2), BF),
            pltpu.VMEM((rest, master, own_columns), BF),
            pltpu.VMEM((rest, master, own_columns), BF),
            pltpu.VMEM((rest, master, own_columns), BF),
            pltpu.VMEM((2, rest - 1, master, own_columns // 2), BF),
            pltpu.VMEM((master, own_columns), BF),
            pltpu.VMEM((count - 1, slab, width), BF),
            pltpu.VMEM((count - 1, slab, width), BF),
            pltpu.VMEM(sums.shape, F32),
            pltpu.VMEM((groups - 1, sums.shape[0], master), F32),
            pltpu.VMEM((sums.shape[0], master), F32),
            pltpu.VMEM((count - 1, sums.shape[0], master), F32),
            dma((3,)),
            dma((count - 1, 2)),
            dma((count - 1, 2)),
            dma((rest,)),
            dma((rest,)),
            dma((2, rest - 1)),
            dma((2, rest - 1)),
            dma((count - 1, 3)),
            dma((count - 1, 3)),
        ]
        + [dma((count - 1,))] * 4
        + [dma((groups - 1,))] * 2
        + [dma((count - 1,))] * 2,
        compiler_params=pltpu.CompilerParams(
            collective_id=call, has_side_effects=True, vmem_limit_bytes=67043328
        ),
        cost_estimate=SHORT,
        name="tail",
    )(grads, dense, hidden, output_sum, normed, sums)


def finish_kernel(*refs):
    in1, down1a, down1b, in2, down2a, down2b = refs[:6]
    dense, (out_in, out_down), dense_out = refs[6:10], refs[10:12], refs[12:]
    ff = out_in.shape[2] // 2
    for pair, value in enumerate((in1, in2)):
        for part in range(2):
            for j in range(PAIR):
                at = (PAIR * (1 + part) + j) * ff
                out_in[:, pair * PAIR + j, part * ff : (part + 1) * ff] = value[:, at : at + ff].astype(F32)
    for i, value in enumerate((down1a, down1b, down2a, down2b)):
        out_down[:, i, :] = value[...].astype(F32)
    for value, out in zip(dense, dense_out):
        out[...] = value[...].astype(F32)


def finish_grads(sum1, sum2, dense):
    master, columns = sum1.shape
    width = columns // 3
    steps = master // PREP_ROWS
    rows = PREP_ROWS // PAIR
    local = 2 * PAIR
    specs = [pl.BlockSpec((PREP_ROWS, columns), lambda i: (i, 0))]
    specs += [pl.BlockSpec((rows, width), lambda i, j=j: (j * steps + i, 0)) for j in range(PAIR)]
    whole = [pl.BlockSpec((PREP_ROWS, width), lambda i: (i, 0))] * len(dense)
    return pl.pallas_call(
        finish_kernel,
        grid=(steps,),
        in_specs=specs * 2 + whole,
        out_specs=[
            pl.BlockSpec((PREP_ROWS, local, width), lambda i: (i, 0, 0)),
            pl.BlockSpec((rows, local, width), lambda i: (i, 0, 0)),
        ]
        + whole,
        out_shape=[
            jax.ShapeDtypeStruct((master, local, width), F32),
            jax.ShapeDtypeStruct((master // PAIR, local, width), F32),
        ]
        + [jax.ShapeDtypeStruct((master, width), F32)] * len(dense),
        cost_estimate=SHORT,
        name="finish",
    )(sum1, sum1, sum1, sum2, sum2, sum2, *dense)


def key_limit(block):
    return max((block + 1) * QBLOCK, MAX_PREFIX)


def visible(block, limit, prefix):
    row = block * QBLOCK + lax.broadcasted_iota(jnp.int32, (QBLOCK, limit), 0)
    col = lax.broadcasted_iota(jnp.int32, (QBLOCK, limit), 1)
    return (col <= row) | (col < prefix)


def attend_kernel(prefix_ref, ql, kl, vb, sq, sk, gq, gk, cos, sin, ob, qb, kb, lse):
    prefix = prefix_ref[0]
    c, s = cos[...], sin[...]
    qn = ql[...] * sq[...] * gq[...]
    kn = kl[...] * sk[...] * gk[...]
    half = HEAD_DIM // 2
    qb[...] = ((qn * c + pltpu.roll(qn, half, 1) * s) * HEAD_DIM ** (-0.5)).astype(BF)
    kb[...] = (kn * c + pltpu.roll(kn, half, 1) * s).astype(BF)
    for block in range(LEN // QBLOCK):
        rows = slice(block * QBLOCK, (block + 1) * QBLOCK)
        limit = key_limit(block)
        scores = dot_nt(qb[rows, :], kb[:limit, :])
        scores = jnp.where(visible(block, limit, prefix), scores, -1e30)
        peak = jnp.max(scores, -1, keepdims=True)
        expo = jnp.exp(scores - peak)
        total = jnp.sum(expo, -1, keepdims=True)
        ob[rows, :] = (dot(expo.astype(BF), vb[:limit, :]) / total).astype(BF)
        lse[0, rows, :] = peak + jnp.log(total)


def attend(prefix, ql, kl, vb, sq, sk, gq, gk, cos, sin):
    heads = ql.shape[1] // HEAD_DIM
    col = pl.BlockSpec((LEN, HEAD_DIM), lambda h, p: (0, h))
    one = pl.BlockSpec((LEN, 1), lambda h, p: (0, 0))
    gain = pl.BlockSpec((1, HEAD_DIM), lambda h, p: (0, h))
    table = pl.BlockSpec((LEN, HEAD_DIM), lambda h, p: (0, 0))
    return pl.pallas_call(
        attend_kernel,
        out_shape=[jax.ShapeDtypeStruct(ql.shape, BF)] * 3
        + [jax.ShapeDtypeStruct((heads, LEN, 1), F32)],
        grid_spec=pltpu.PrefetchScalarGridSpec(
            num_scalar_prefetch=1,
            grid=(heads,),
            in_specs=[col, col, col, one, one, gain, gain, table, table],
            out_specs=[col, col, col, pl.BlockSpec((1, LEN, 1), lambda h, p: (h, 0, 0))],
        ),
        cost_estimate=SHORT,
        name="attend",
    )(prefix, ql, kl, vb, sq, sk, gq, gk, cos, sin)


def attend_back_kernel(
    prefix_ref, qb, kb, vb, dob, lse, ql, kl, sq, sk, gq, gk, cos, sin,
    wq, wk, dv, inner, gain_q, gain_k, dq_sum, dk_sum, dv_sum,
):
    prefix = prefix_ref[0]
    dk_sum[...] = jnp.zeros_like(dk_sum)
    dv_sum[...] = jnp.zeros_like(dv_sum)
    for block in range(LEN // QBLOCK):
        rows = slice(block * QBLOCK, (block + 1) * QBLOCK)
        limit = key_limit(block)
        scores = dot_nt(qb[rows, :], kb[:limit, :])
        weights = jnp.where(visible(block, limit, prefix), jnp.exp(scores - lse[0, rows, :]), 0.0)
        grad = dob[rows, :]
        dweights = dot_nt(grad, vb[:limit, :])
        dscores = (weights * (dweights - jnp.sum(dweights * weights, -1, keepdims=True))).astype(BF)
        dq_sum[rows, :] = dot(dscores, kb[:limit, :])
        dk_sum[:limit, :] += dot_tn(dscores, qb[rows, :])
        dv_sum[:limit, :] += dot_tn(weights.astype(BF), grad)
    dv[...] = dv_sum[...].astype(BF)
    c, s = cos[...], sin[...]
    half = HEAD_DIM // 2
    dq = dq_sum[...] * HEAD_DIM ** (-0.5)
    dqn = dq * c - pltpu.roll(dq, half, 1) * s
    dk = dk_sum[...]
    dkn = dk * c - pltpu.roll(dk, half, 1) * s
    gain_q[...] = jnp.sum(dqn * (ql[...] * sq[...]), 0, keepdims=True)
    gain_k[...] = jnp.sum(dkn * (kl[...] * sk[...]), 0, keepdims=True)
    dqn = dqn * gq[...]
    dkn = dkn * gk[...]
    wq[...] = dqn
    wk[...] = dkn
    part = jnp.concatenate(
        [jnp.sum(dqn * ql[...], -1, keepdims=True), jnp.sum(dkn * kl[...], -1, keepdims=True)], 1
    )

    @pl.when(pl.program_id(0) == 0)
    def _():
        inner[...] = part

    @pl.when(pl.program_id(0) > 0)
    def _():
        inner[...] += part


def attend_back(prefix, qb, kb, vb, dob, lse, ql, kl, sq, sk, gq, gk, cos, sin):
    heads = ql.shape[1] // HEAD_DIM
    col = pl.BlockSpec((LEN, HEAD_DIM), lambda h, p: (0, h))
    one = pl.BlockSpec((LEN, 1), lambda h, p: (0, 0))
    gain = pl.BlockSpec((1, HEAD_DIM), lambda h, p: (0, h))
    table = pl.BlockSpec((LEN, HEAD_DIM), lambda h, p: (0, 0))
    return pl.pallas_call(
        attend_back_kernel,
        out_shape=[
            jax.ShapeDtypeStruct(ql.shape, F32),
            jax.ShapeDtypeStruct(ql.shape, F32),
            jax.ShapeDtypeStruct(ql.shape, BF),
            jax.ShapeDtypeStruct((LEN, 2), F32),
            jax.ShapeDtypeStruct((1, ql.shape[1]), F32),
            jax.ShapeDtypeStruct((1, ql.shape[1]), F32),
        ],
        grid_spec=pltpu.PrefetchScalarGridSpec(
            num_scalar_prefetch=1,
            grid=(heads,),
            in_specs=[col, col, col, col, pl.BlockSpec((1, LEN, 1), lambda h, p: (h, 0, 0)),
                      col, col, one, one, gain, gain, table, table],
            out_specs=[col, col, col, pl.BlockSpec((LEN, 2), lambda h, p: (0, 0)), gain, gain],
            scratch_shapes=[pltpu.VMEM((LEN, HEAD_DIM), F32)] * 3,
        ),
        cost_estimate=SHORT,
        name="attend_back",
    )(prefix, qb, kb, vb, dob, lse, ql, kl, sq, sk, gq, gk, cos, sin)


FTILE = 256
PAIR = 2


def expert_kernel(first, b, c, wg, wu, wd, gates, hg, dg, du, dgate):
    lanes = lax.broadcasted_iota(jnp.int32, gates.shape, 1) == first[0] + pl.program_id(0)
    g = dot(b[...], wg[...])
    u = dot(b[...], wu[...])
    back = dot_nt(c[...], wd[...].reshape(FTILE, wd.shape[-1]))
    sigma = jax.nn.sigmoid(g)
    silu = g * sigma
    h = silu * u
    weight = jnp.sum(jnp.where(lanes, gates[...], 0.0), -1, keepdims=True)
    hidden = (weight * h).astype(BF)
    block = hg.shape[3]
    for i in range(hg.shape[0]):
        hg[i, 0] = hidden[:, i * block : (i + 1) * block]
    part = jnp.where(lanes, jnp.sum(h * back, -1, keepdims=True), 0.0)
    dh = weight * back
    dg[...] = (dh * u * (sigma * (1.0 + g * (1.0 - sigma)))).astype(BF)
    du[...] = (dh * silu).astype(BF)
    start = (pl.program_id(0) == 0) & (pl.program_id(1) == 0)

    @pl.when(start)
    def _():
        dgate[...] = part

    @pl.when(jnp.logical_not(start))
    def _():
        dgate[...] += part


def experts(first, b, c, weights, gates, ff):
    rows, width = b.shape
    tiles = ff // FTILE
    block = weights.shape[2]
    whole = pl.BlockSpec((rows, width), lambda j, f, p: (0, 0), pipeline_mode=pl.Buffered(1))
    one = pl.BlockSpec((rows, LANES), lambda j, f, p: (0, 0))
    out = pl.BlockSpec((rows, FTILE), lambda j, f, p: (0, j * tiles + f))
    flat = weights.reshape(width, weights.shape[3])
    return pl.pallas_call(
        expert_kernel,
        grid_spec=pltpu.PrefetchScalarGridSpec(
            num_scalar_prefetch=1,
            grid=(PAIR, tiles),
            in_specs=[
                whole,
                whole,
                pl.BlockSpec((width, FTILE), lambda j, f, p: (0, j * tiles + f)),
                pl.BlockSpec((width, FTILE), lambda j, f, p: (0, (PAIR + j) * tiles + f)),
                pl.BlockSpec((FTILE // block, 1, block, width), lambda j, f, p: (f, j, 0, 2)),
                one,
            ],
            out_specs=[
                pl.BlockSpec((FTILE // block, 1, rows, block), lambda j, f, p: (f, j, 0, 0)),
                out,
                out,
                one,
            ],
        ),
        out_shape=[jax.ShapeDtypeStruct((ff // block, PAIR, rows, block), BF)]
        + [jax.ShapeDtypeStruct((rows, PAIR * ff), BF)] * 2
        + [jax.ShapeDtypeStruct((rows, LANES), F32)],
        cost_estimate=SHORT,
        name="experts",
    )(first, b, c, flat, flat, weights, gates)


NTILE = 256
GROUPS = 8
STEP_BACK, STEP_DOWN, LINK_US, HOP_US = 5.4, 2.8, 2.85, 3.5


def ring_steps(count, tiles, last):
    per = tiles // GROUPS
    ends, now = [], 0.0
    for step in range(last + 1):
        now += STEP_BACK if step < tiles else STEP_DOWN
        ends.append(now)
    steps, ready, free = {}, {(GROUPS, 0): 0.0}, 0.0
    pending = []
    for step in range(last + 1):
        if step < tiles and step % per == per - 1:
            ready[step // per, 0] = ends[step]
        while ready:
            action = min(ready, key=lambda key: (ready[key], key))
            if ready[action] > ends[step] and step < last:
                break
            at = max(ready.pop(action), ends[step])
            steps.setdefault(step, []).append(action)
            group, hop = action
            if hop < count - 1:
                free = max(free, at) + LINK_US
                ready[group, hop + 1] = free + HOP_US
    return steps


def middle_kernel(
    count, tiles, steps, dg1, du1, dg2, du2, hg1, hg2, probs, wg1, wu1, wg2, wu2, wd1, wd2,
    back_out, partial,
    held1, held2, held3, held4, hidden1, hidden2, back, sent, landed, probs_sent, probs_landed,
    load_sem, send_sem, recv_sem,
):
    step = pl.program_id(0)
    here = lax.axis_index("expert")
    right, left = lax.rem(here + 1, count), lax.rem(here + count - 1, count)
    columns = tiles * NTILE
    lanes = columns // GROUPS
    rows = back.shape[0] // count
    loads = [
        pltpu.make_async_copy(source, target, load_sem.at[i])
        for i, (source, target) in enumerate(
            (
                (dg1, held1), (du1, held2), (dg2, held3), (du2, held4),
                (hg1, hidden1), (hg2, hidden2),
            )
        )
    ]

    @pl.when(step == 0)
    def _():
        barrier = pltpu.get_barrier_semaphore()
        for other in (left, right):
            pl.semaphore_signal(barrier, inc=1, device_id={"expert": other}, device_id_type=MESH)
        for load in loads:
            load.start()
        pl.semaphore_wait(barrier, 2)
        total = None
        for i, (left_ref, right_ref) in enumerate(((held1, wg1), (held2, wu1), (held3, wg2), (held4, wu2))):
            loads[i].wait()
            term = dot_nt(left_ref[...], right_ref[...])
            total = term if total is None else total + term
        back[:, :NTILE] = total.astype(BF)

    @pl.when((step > 0) & (step < tiles))
    def _():
        total = (
            dot_nt(held1[...], wg1[...])
            + dot_nt(held2[...], wu1[...])
            + dot_nt(held3[...], wg2[...])
            + dot_nt(held4[...], wu2[...])
        )
        back[:, pl.ds(pl.multiple_of(step * NTILE, NTILE), NTILE)] = total.astype(BF)

    @pl.when(step == tiles)
    def _():
        loads[4].wait()
        loads[5].wait()

    @pl.when(step >= tiles)
    def _():
        total = None
        for hidden, weight in ((hidden1, wd1), (hidden2, wd2)):
            for j in range(PAIR):
                left_value = jnp.concatenate([hidden[i, j] for i in range(hidden.shape[0])], -1)
                term = dot(left_value, weight[:, j].reshape(left_value.shape[1], NTILE))
                total = term if total is None else total + term
        partial[...] = total.astype(BF)

    def copy(group, hop):
        source, target = (sent, landed) if group < GROUPS else (probs_sent, probs_landed)
        at = (hop, group) if group < GROUPS else (hop,)
        return pltpu.make_async_remote_copy(
            src_ref=source.at[at], dst_ref=target.at[at],
            send_sem=send_sem.at[hop, group], recv_sem=recv_sem.at[hop, group],
            device_id={"expert": right}, device_id_type=MESH,
        )

    def advance(group, hop):
        at = (slice(group * lanes, (group + 1) * lanes) if group < GROUPS else slice(columns, columns + LANES))
        block = pl.ds(pl.multiple_of(lax.rem(here - 1 - hop + count, count) * rows, rows), rows)
        total = (back[block, at] if group < GROUPS else probs[block, :]).astype(F32)
        if hop:
            copy(group, hop - 1).wait_recv()
            total = total + (landed[hop - 1, group] if group < GROUPS else probs_landed[hop - 1]).astype(F32)
        if hop == count - 1:
            back_out[:, at] = total
            return
        if group < GROUPS:
            sent[hop, group] = total.astype(BF)
        else:
            probs_sent[hop] = total.astype(BF)
        copy(group, hop).start()

    for at, actions in steps.items():

        @pl.when(step == at)
        def _():
            for group, hop in actions:
                advance(group, hop)

    @pl.when(step == pl.num_programs(0) - 1)
    def _():
        for hop in range(count - 1):
            for group in range(GROUPS + 1):
                copy(group, hop).wait_send()


def middle(pair1, pair2, probs, weights1, weights2, count, call):
    (hg1, dg1, du1), (hg2, dg2, du2) = pair1, pair2
    devices, _, rows, block = hg1.shape
    width = devices * PAIR * block
    tiles = width // NTILE
    flat1, flat2 = [w.reshape(width, w.shape[3]) for w in (weights1, weights2)]
    anywhere = pl.BlockSpec(memory_space=pl.ANY)
    gate = pl.BlockSpec((NTILE, width), lambda s: (jnp.minimum(s, tiles - 1), 0))
    up = pl.BlockSpec((NTILE, width), lambda s: (jnp.minimum(s, tiles - 1), 1))
    second = lambda s: jnp.clip(s - tiles, 0, tiles - 1)
    weight = pl.BlockSpec((devices, PAIR, block, NTILE), lambda s: (0, 0, 0, 2 * width // NTILE + second(s)))
    dma = pltpu.SemaphoreType.DMA
    lanes = width // GROUPS
    return pl.pallas_call(
        functools.partial(middle_kernel, count, tiles, ring_steps(count, tiles, 2 * tiles - 1)),
        grid=(2 * tiles,),
        in_specs=[anywhere] * 6
        + [pl.BlockSpec((rows, LANES), lambda s: (0, 0), pipeline_mode=pl.Buffered(1))]
        + [gate, up, gate, up, weight, weight],
        out_specs=[
            pl.BlockSpec((rows // count, width + LANES), lambda s: (0, 0), pipeline_mode=pl.Buffered(1)),
            pl.BlockSpec((rows, NTILE), lambda s: (0, second(s))),
        ],
        out_shape=[
            jax.ShapeDtypeStruct((rows // count, width + LANES), F32),
            jax.ShapeDtypeStruct((rows, width), BF),
        ],
        scratch_shapes=[pltpu.VMEM((rows, width), BF)] * 4
        + [pltpu.VMEM(hg1.shape, BF)] * 2
        + [
            pltpu.VMEM((rows, width), BF),
            pltpu.VMEM((count - 1, GROUPS, rows // count, lanes), BF),
            pltpu.VMEM((count - 1, GROUPS, rows // count, lanes), BF),
            pltpu.VMEM((count - 1, rows // count, LANES), BF),
            pltpu.VMEM((count - 1, rows // count, LANES), BF),
            dma((6,)),
            dma((count - 1, GROUPS + 1)),
            dma((count - 1, GROUPS + 1)),
        ],
        compiler_params=pltpu.CompilerParams(
            collective_id=call, has_side_effects=True, vmem_limit_bytes=67043328
        ),
        cost_estimate=SHORT,
        name="middle",
    )(dg1, du1, dg2, du2, hg1, hg2, probs, flat1, flat1, flat2, flat2, weights1, weights2)


def body(
    tokens,
    routes,
    prefix,
    query_weight,
    key_weight,
    value_weight,
    output_weight,
    router_weight,
    attention_gain,
    feedforward_gain,
    query_gain,
    key_gain,
    expert_in,
    expert_down,
    cotangent,
):
    count = lax.axis_size("expert")
    here = lax.axis_index("expert")
    rows, width = tokens.shape
    cols = width // count
    experts_all = router_weight.shape[1]
    local = expert_in.shape[1]
    ff_rows = expert_down.shape[0]
    ff = expert_in.shape[2] // 2
    master = query_weight.shape[0]

    def gather(value):
        return lax.all_gather(value, "group", axis=0, tiled=True)

    cores = [list(range(core, width // master, 2)) for core in range(2)]

    def scatter_all(value):
        return lax.psum_scatter(value, "group", scatter_dimension=0, tiled=True)

    def scatter(value):
        return lax.psum_scatter(value, "group", scatter_dimension=0, tiled=True, axis_index_groups=cores)

    def own_cols(weight):
        return lax.dynamic_slice(weight, (0, here * cols), (master, cols)).astype(BF)

    small = jnp.concatenate(
        [
            jnp.pad(router_weight, ((0, 0), (0, LANES // 2 - experts_all))),
            jnp.stack([attention_gain, feedforward_gain, query_gain, key_gain], 1),
            jnp.zeros((master, LANES // 2 - 4), F32),
        ],
        1,
    ).astype(BF)
    dense = gather(
        jnp.concatenate(
            [own_cols(query_weight), own_cols(key_weight), own_cols(value_weight), output_weight.astype(BF), small],
            1,
        )
    )
    qkv_weight = dense[:, : 3 * cols]
    out_weight = dense[:, 3 * cols : 3 * cols + width]
    router = dense[:, 3 * cols + width :]
    gains = router[:, LANES // 2 :].astype(F32).T
    gain_one, gain_two = gains[0:1], gains[1:2]
    gain_query = lax.dynamic_slice(gains[2:3], (0, here * cols), (1, cols))
    gain_key = lax.dynamic_slice(gains[3:4], (0, here * cols), (1, cols))

    expert_ids = jnp.arange(experts_all, dtype=jnp.int32)
    selected = jnp.sum((routes[:, :, None] == expert_ids).astype(F32), 1)
    sent = jnp.concatenate(
        [tokens, jnp.pad(selected, ((0, 0), (0, LANES - experts_all))).astype(BF)], 1
    )
    sent, own1, own2 = gather_and_prep(sent, expert_in, expert_down, count, 2)
    weights1, weights2 = [gather(own).reshape(-1, PAIR, ff_rows, own.shape[1]) for own in (own1, own2)]
    x_all = sent[:, :width].astype(F32)
    chosen = sent[:, width:].astype(F32)

    steps = jnp.arange(HEAD_DIM // 2).astype(F32)
    freq = jnp.exp(steps * (-2.0 * math.log(THETA) / HEAD_DIM))
    angle = jnp.arange(LEN).astype(F32)[:, None] * freq[None, :]
    cosine = jnp.concatenate([jnp.cos(angle)] * 2, 1)
    sine = jnp.concatenate([-jnp.sin(angle), jnp.sin(angle)], 1)

    hidden_one = (x_all * row_scale(x_all) * gain_one).astype(BF)
    cot_blocks = [cotangent]

    def cot_hop(value, *done):
        if len(cot_blocks) < count:
            cot_blocks.append(shift(after(cot_blocks[-1], *done), count, 1))
            value = after(value, cot_blocks[-1])
        return value

    hidden_one = cot_hop(hidden_one, sent)
    qkv = dot(hidden_one, qkv_weight)
    query_lin, key_lin = qkv[:, :cols], qkv[:, cols : 2 * cols]
    value_bf = qkv[:, 2 * cols :].astype(BF)
    value_bf = cot_hop(value_bf)
    squares = jnp.stack([jnp.sum(query_lin * query_lin, -1), jnp.sum(key_lin * key_lin, -1)])
    scales = exchange_sum(after(squares, value_bf), count, 0)
    between = scales
    scales = lax.rsqrt(scales / width + EPS)
    scale_query, scale_key = scales[0][:, None], scales[1][:, None]
    attended, query_bf, key_bf, lse = attend(
        prefix, query_lin, key_lin, value_bf, scale_query, scale_key, gain_query, gain_key, cosine, sine
    )
    attended_bf = heads_to_rows(cot_hop(attended, between), count, 4)

    xfloat = tokens.astype(F32)
    resid = xfloat + dot(attended_bf, out_weight)
    scale_two = row_scale(resid)
    normed_two = resid * scale_two
    hidden_two = (normed_two * gain_two).astype(BF)
    while len(cot_blocks) < count:
        hidden_two = cot_hop(hidden_two, attended_bf)
    b_all, = gather_rows((hidden_two,), count, 3)
    cot_all = jnp.zeros((LEN, width), BF)
    for step, block in enumerate(cot_blocks):
        cot_all = lax.dynamic_update_slice(cot_all, block, (((here - step) % count) * rows, 0))

    def route(value):
        lanes = lax.broadcasted_iota(jnp.int32, (1, LANES), 1)
        return jax.nn.softmax(jnp.where(lanes < experts_all, dot(value, router), -1e30), -1)

    gates = route(b_all) * chosen
    own_probs = route(hidden_two)
    first = jnp.full((1,), here * local, jnp.int32)
    devices = width // master
    hg1, dg1, du1, dgate1 = experts(first, b_all, cot_all, weights1, gates, ff)
    term1, = grad_terms(hg1, b_all, cot_all, dg1, du1, 9)
    sum1 = scatter(term1)
    hg2, dg2, du2, dgate2 = experts(first + PAIR, after(b_all, term1), cot_all, weights2, gates, ff)
    dprobs = (dgate1 + dgate2) * chosen

    back, partial = middle((hg1, dg1, du1), (hg2, dg2, du2), dprobs, weights1, weights2, count, 8)
    grad_probs = back[:, width:]
    grad_logits = (
        own_probs * (grad_probs - jnp.sum(grad_probs * own_probs, -1, keepdims=True))
    ).astype(BF)
    grad_router = dot_tn(grad_logits, hidden_two)[:experts_all]
    grad_two = back[:, :width] + dot_nt(grad_logits, router)
    gain_two_term = jnp.sum(grad_two * normed_two, 0)
    grad_out = cotangent.astype(F32)
    grad_resid = grad_out + norm_back(resid, scale_two, grad_two * gain_two)
    grad_attn_out = grad_resid.astype(BF)
    output_term = dot_tn(attended_bf, grad_attn_out).astype(BF)
    output_sum = scatter_all(output_term)
    term2, first_out, heads_grad = grad_terms(
        hg2, b_all, cot_all, dg2, after(du2, output_term), 10, partial, grad_attn_out, dense, count
    )
    sum2 = scatter(term2)
    ring_out = Ring(partial, first_out, count, here)

    wq, wk, dvl, inner, gain_q_term, gain_k_term = attend_back(
        prefix, query_bf, key_bf, value_bf, heads_grad, lse, query_lin, key_lin,
        scale_query, scale_key, gain_query, gain_key, cosine, sine,
    )
    last = ring_out.hop(inner)
    inner = exchange_sum(after(inner, last).T, count, 1) / width
    ring_out.total = after(ring_out.total, inner)
    dql = scale_query * wq - query_lin * (scale_query**3 * inner[0][:, None])
    dkl = scale_key * wk - key_lin * (scale_key**3 * inner[1][:, None])
    dqkv = jnp.concatenate([dql.astype(BF), dkl.astype(BF), dvl], 1)

    def spread(value):
        return lax.dynamic_update_slice(jnp.zeros((1, width), F32), value, (0, here * cols))

    scale_one = row_scale(xfloat)
    sums = jnp.concatenate(
        [
            jnp.zeros((1, width), F32),
            gain_two_term[None],
            spread(gain_q_term),
            spread(gain_k_term),
            jnp.zeros((4, width), F32),
            grad_router,
        ]
    )
    grad_hidden, *dense_grads, sums = tail(
        after(dqkv, sum1), dense, hidden_one, output_sum, xfloat * scale_one, sums, count, devices, 6
    )

    output = (resid + ring_out.finish(grad_hidden)).astype(BF)
    grad_tokens = grad_resid + norm_back(xfloat, scale_one, grad_hidden * gain_one)
    grad_in, grad_down, grad_q, grad_k, grad_v, grad_out_weight = finish_grads(sum1, sum2, dense_grads)
    return (
        output,
        grad_tokens,
        grad_q,
        grad_k,
        grad_v,
        grad_out_weight,
        sums[8:].T,
        sums[0],
        sums[1],
        sums[2],
        sums[3],
        grad_in,
        grad_down,
    )


def solution(mesh):
    in_specs = (
        P(("group", "expert"), None),
        P(("group", "expert"), None),
        P("group"),
        P("group", None),
        P("group", None),
        P("group", None),
        P("group", None),
        P("group", None),
        P("group"),
        P("group"),
        P("group"),
        P("group"),
        P("group", "expert", None),
        P("group", "expert", None),
        P(("group", "expert"), None),
    )
    out_specs = (
        P(("group", "expert"), None),
        P(("group", "expert"), None),
        P("group", None),
        P("group", None),
        P("group", None),
        P("group", None),
        P("group", None),
        P("group"),
        P("group"),
        P("group"),
        P("group"),
        P("group", "expert", None),
        P("group", "expert", None),
    )
    return jax.shard_map(body, mesh=mesh, in_specs=in_specs, out_specs=out_specs, check_vma=False)
```

```python
import functools
import math

import jax
import jax.numpy as jnp
from jax import lax
from jax.experimental import pallas as pl
from jax.experimental.pallas import tpu as pltpu
from jax.sharding import PartitionSpec as P

HEADS = 16
HEAD_DIM = 128
LEN = 1024
MAX_PREFIX = LEN // 2
QBLOCK = 256
EPS = 1e-05
THETA = 10000.0
BF = jnp.bfloat16
F32 = jnp.float32
MESH = pl.DeviceIdType.MESH
LANES = 128
SHORT = pl.CostEstimate(flops=1000000, bytes_accessed=1000000, transcendentals=0)


def dot(left, right):
    return jnp.dot(left, right, preferred_element_type=F32)


def dot_nt(left, right):
    return lax.dot_general(left, right, (((1,), (1,)), ((), ())), preferred_element_type=F32)


def dot_tn(left, right):
    return lax.dot_general(left, right, (((0,), (0,)), ((), ())), preferred_element_type=F32)


def row_scale(values):
    return lax.rsqrt(jnp.mean(values * values, -1, keepdims=True) + EPS)


def norm_back(values, scale_rows, upstream):
    inner = jnp.mean(upstream * values, -1, keepdims=True)
    return scale_rows * upstream - values * (scale_rows * scale_rows * scale_rows) * inner


def shift(value, count, step):
    return lax.ppermute(value, "expert", [(i, (i + step) % count) for i in range(count)])


class Ring:
    def __init__(self, value, arrived, count, here):
        self.value, self.count, self.here = value, count, here
        self.step = 1
        self.total = self.term() + arrived.astype(F32)

    def term(self):
        rows = self.value.shape[0] // self.count
        block = (self.here - 1 - self.step) % self.count
        return lax.dynamic_slice(self.value, (block * rows, 0), (rows, self.value.shape[1]))

    def hop(self, *done):
        arrived = shift(self.total.astype(BF), self.count, 1)
        self.step += 1
        self.total = self.term() + after(arrived, *done).astype(F32)
        return self.total

    def finish(self, *done):
        while self.step < self.count - 1:
            self.hop(*done)
        return self.total


def exchange_kernel(count, value, out, slots, send_sem, recv_sem):
    here = lax.axis_index("expert")
    others = [lax.rem(here + step, count) for step in range(1, count)]
    barrier = pltpu.get_barrier_semaphore()
    for other in others:
        pl.semaphore_signal(barrier, inc=1, device_id={"expert": other}, device_id_type=MESH)
    pl.semaphore_wait(barrier, count - 1)
    copies = [
        pltpu.make_async_remote_copy(
            src_ref=value,
            dst_ref=slots.at[i],
            send_sem=send_sem.at[i],
            recv_sem=recv_sem.at[i],
            device_id={"expert": other},
            device_id_type=MESH,
        )
        for i, other in enumerate(others)
    ]
    for copy in copies:
        copy.start()
    for copy in copies:
        copy.wait()
    total = value[...]
    for i in range(count - 1):
        total = total + slots[i]
    out[...] = total


def exchange_sum(value, count, call):
    return pl.pallas_call(
        functools.partial(exchange_kernel, count),
        out_shape=jax.ShapeDtypeStruct(value.shape, F32),
        in_specs=[pl.BlockSpec(memory_space=pltpu.VMEM)],
        out_specs=pl.BlockSpec(memory_space=pltpu.VMEM),
        scratch_shapes=[
            pltpu.VMEM((count - 1,) + value.shape, F32),
            pltpu.SemaphoreType.DMA((count - 1,)),
            pltpu.SemaphoreType.DMA((count - 1,)),
        ],
        compiler_params=pltpu.CompilerParams(collective_id=call, has_side_effects=True),
        name="exchange%d" % call,
    )(value)


def after(value, *done):
    return lax.optimization_barrier((value,) + done)[0]


PIECES = 2


def gather_kernel(count, arrays, *refs):
    values, wholes = refs[:arrays], refs[arrays : 2 * arrays]
    local, sems = refs[2 * arrays : 3 * arrays], refs[3 * arrays :]
    send_sem, recv_sem, in_sem, out_sem = sems
    here = lax.axis_index("expert")
    right, left = lax.rem(here + 1, count), lax.rem(here + count - 1, count)
    other_core = flipped(lax.axis_index("group"), 1)

    def hop(array, step, piece):
        rows = values[array].shape[0]
        size = rows // PIECES
        owner = lax.rem(here - step + count, count)
        place = wholes[array].at[pl.ds(pl.multiple_of(owner * rows + piece * size, size), size)]
        return pltpu.make_async_remote_copy(
            src_ref=place if step else values[array].at[pl.ds(piece * size, size)],
            dst_ref=place,
            send_sem=send_sem.at[array, step, piece],
            recv_sem=recv_sem.at[array, step, piece],
            device_id={"expert": right},
            device_id_type=MESH,
        )

    loads = [pltpu.make_async_copy(values[i], local[i], in_sem.at[i]) for i in range(arrays)]

    @pl.when(pl.program_id(0) == 0)
    def _():
        barrier = pltpu.get_barrier_semaphore()
        for other in (left, right):
            pl.semaphore_signal(barrier, inc=1, device_id={"expert": other}, device_id_type=MESH)
        pl.semaphore_signal(barrier, inc=1, device_id={"group": other_core}, device_id_type=MESH)
        pl.semaphore_wait(barrier, 3)
        for i in range(arrays):
            for piece in range(PIECES):
                hop(i, 0, piece).start()
            loads[i].start()

    def rest():
        stores = []
        for i in range(arrays):
            rows = values[i].shape[0]
            loads[i].wait()
            stores.append(
                pltpu.make_async_copy(
                    local[i], wholes[i].at[pl.ds(pl.multiple_of(here * rows, rows), rows)], out_sem.at[i]
                )
            )
            stores[i].start()
        for i in range(arrays):
            for step in range(1, count - 1):
                for piece in range(PIECES):
                    hop(i, step - 1, piece).wait_recv()
                    hop(i, step, piece).start()
        for i in range(arrays):
            stores[i].wait()
            for piece in range(PIECES):
                hop(i, count - 2, piece).wait_recv()
                for step in range(count - 1):
                    hop(i, step, piece).wait_send()

    return rest


def gather_only(count, arrays, *refs):
    gather_kernel(count, arrays, *refs)()


def gather_scratch(values, count):
    arrays = len(values)
    hops = pltpu.SemaphoreType.DMA((arrays, count - 1, PIECES))
    return [pltpu.VMEM(v.shape, v.dtype) for v in values] + [
        hops, hops, pltpu.SemaphoreType.DMA((arrays,)), pltpu.SemaphoreType.DMA((arrays,))
    ]


def gather_rows(values, count, call):
    arrays = len(values)
    return pl.pallas_call(
        functools.partial(gather_only, count, arrays),
        grid=(1,),
        out_shape=[jax.ShapeDtypeStruct((count * v.shape[0],) + v.shape[1:], v.dtype) for v in values],
        in_specs=[pl.BlockSpec(memory_space=pl.ANY)] * arrays,
        out_specs=[pl.BlockSpec(memory_space=pl.ANY)] * arrays,
        scratch_shapes=gather_scratch(values, count),
        compiler_params=pltpu.CompilerParams(collective_id=call, has_side_effects=True),
        cost_estimate=SHORT,
        name="gather%d" % call,
    )(*values)


PREP_ROWS = 32


def prep_kernel(count, halves, value, up, lower, whole, out1, out2, *scratch):
    rest = gather_kernel(count, 1, value, whole, *scratch)
    ff = up.shape[2] // 2
    for pair, out in enumerate((out1, out2)):
        for j in range(PAIR):
            row = up[:, pair * PAIR + j, :].astype(BF)
            out[:, j * ff : (j + 1) * ff] = row[:, :ff]
            out[:, (PAIR + j) * ff : (PAIR + j + 1) * ff] = row[:, ff:]

        for j in range(PAIR):

            @pl.when(pl.program_id(0) // halves == j)
            def _():
                out[:, 2 * PAIR * ff :] = lower[:, pair * PAIR + j, :].astype(BF)

    pl.when(pl.program_id(0) == pl.num_programs(0) - 1)(rest)


def gather_and_prep(value, expert_in, expert_down, count, call):
    master, local, both = expert_in.shape
    halves = expert_down.shape[0] // PREP_ROWS
    width = expert_down.shape[2]
    columns = PAIR * both + width
    anywhere = pl.BlockSpec(memory_space=pl.ANY)
    return pl.pallas_call(
        functools.partial(prep_kernel, count, halves),
        grid=(master // PREP_ROWS,),
        in_specs=[
            anywhere,
            pl.BlockSpec((PREP_ROWS, local, both), lambda i: (i, 0, 0)),
            pl.BlockSpec((PREP_ROWS, local, width), lambda i: (lax.rem(i, halves), 0, 0)),
        ],
        out_specs=[anywhere] + [pl.BlockSpec((PREP_ROWS, columns), lambda i: (i, 0))] * 2,
        out_shape=[jax.ShapeDtypeStruct((count * value.shape[0],) + value.shape[1:], value.dtype)]
        + [jax.ShapeDtypeStruct((master, columns), BF)] * 2,
        scratch_shapes=gather_scratch((value,), count),
        compiler_params=pltpu.CompilerParams(collective_id=call, has_side_effects=True),
        cost_estimate=SHORT,
        name="gather%d" % call,
    )(value, expert_in, expert_down)


SLOTS = 3


def grads_kernel(count, hg, b, cot, dg, du, *refs):
    if count:
        partial, grad, *refs = refs
        weights, (out, first_in, heads_out), refs = refs[:count], refs[count : count + 3], refs[count + 3 :]
    else:
        out, *refs = refs
    hg_held, b_held, cot_held, dg_held, du_held, sent, landed, sem, send_sem, recv_sem = refs[:10]
    step = pl.program_id(0)
    group = lax.axis_index("group")
    core = lax.rem(group, 2)
    other = flipped(group, 1)
    size, columns = out.shape[0], cot_held.shape[1]
    chips = landed.shape[0]
    loads = [
        pltpu.make_async_copy(source, held, sem.at[i])
        for i, (source, held) in enumerate(
            ((hg, hg_held), (cot, cot_held), (b, b_held), (dg, dg_held), (du, du_held))
        )
    ]

    def copy(chip):
        return pltpu.make_async_remote_copy(
            src_ref=sent.at[lax.rem(chip, SLOTS)], dst_ref=landed.at[chip], send_sem=send_sem.at[chip], recv_sem=recv_sem.at[chip],
            device_id={"group": other}, device_id_type=MESH,
        )

    def terms(place):
        left_down = jnp.concatenate([hg_held[place, j] for j in range(PAIR)], -1)
        left = b_held[:, pl.ds(pl.multiple_of(place * size, size), size)]
        return (left_down, cot_held), (left, dg_held), (left, du_held)

    lanes = [slice(i * columns, (i + 1) * columns) for i in range(3)]
    if count:
        here = lax.axis_index("expert")
        right, left = lax.rem(here + 1, count), lax.rem(here + count - 1, count)
        rows = partial.shape[0] // count
        first = pltpu.make_async_remote_copy(
            src_ref=partial.at[pl.ds(pl.multiple_of(left * rows, rows), rows)], dst_ref=first_in,
            send_sem=refs[10].at[0], recv_sem=refs[10].at[1], device_id={"expert": right}, device_id_type=MESH,
        )
        heads_sent, heads_send, heads_recv, own_sem = refs[11:]
        own_rows, cols = grad.shape[0], heads_out.shape[1]
        others = [lax.rem(here + number, count) for number in range(1, count)]
        own_place = heads_out.at[pl.ds(pl.multiple_of(here * own_rows, own_rows), own_rows)]

        def heads(other):
            at = pl.ds(pl.multiple_of(other * cols, cols), cols)
            total = None
            for i, weight in enumerate(weights):
                term = dot_nt(grad[:, i * cols : (i + 1) * cols], weight[at, :])
                total = term if total is None else total + term
            return total.astype(BF)

        heads_copies = [
            pltpu.make_async_remote_copy(
                src_ref=heads_sent.at[i], dst_ref=own_place, send_sem=heads_send.at[i], recv_sem=heads_recv.at[i],
                device_id={"expert": device}, device_id_type=MESH,
            )
            for i, device in enumerate(others)
        ]

    @pl.when(step == 0)
    def _():
        barrier = pltpu.get_barrier_semaphore()
        pl.semaphore_signal(barrier, inc=1, device_id={"group": other}, device_id_type=MESH)
        if count:
            for device in others:
                pl.semaphore_signal(barrier, inc=1, device_id={"expert": device}, device_id_type=MESH)
        for load in loads:
            load.start()
        pl.semaphore_wait(barrier, count if count else 1)
        if count:
            for i, device in enumerate(others):
                heads_sent[i] = heads(device)
                heads_copies[i].start()
            first.start()
            heads_sent[count - 1] = heads(here)
            own_copy = pltpu.make_async_copy(heads_sent.at[count - 1], own_place, own_sem)
            own_copy.start()
        loads[0].wait()
        loads[2].wait()
        for i, (left_value, right_ref) in enumerate(terms(1 - core)):
            loads[(1, 3, 4)[i]].wait()
            sent[0, :, lanes[i]] = dot_tn(left_value, right_ref[...]).astype(BF)
        copy(0).start()

    @pl.when((step > 0) & (step < chips))
    def _():
        @pl.when(step >= SLOTS)
        def _():
            copy(step - SLOTS).wait_send()

        slot = lax.rem(step, SLOTS)
        for i, (left_value, right_ref) in enumerate(terms(2 * step + 1 - core)):
            sent[slot, :, lanes[i]] = dot_tn(left_value, right_ref[...]).astype(BF)
        copy(step).start()

    @pl.when(step >= chips)
    def _():
        chip = step - chips
        copy(chip).wait_recv()
        for i, (left_value, right_ref) in enumerate(terms(2 * chip + core)):
            total = dot_tn(left_value, right_ref[...]) + landed[chip, :, lanes[i]].astype(F32)
            out[:, lanes[i]] = total.astype(BF)

    @pl.when(step == 2 * chips - 1)
    def _():
        for chip in range(max(chips - SLOTS, 0), chips):
            copy(chip).wait_send()
        if count:
            pltpu.make_async_copy(heads_sent.at[count - 1], own_place, own_sem).wait()
            for copied in heads_copies:
                copied.wait()
            first.wait()


def grad_terms(hg, b, cot, dg, du, call, partial=None, grad=None, dense=None, count=0):
    blocks, _, rows, block = hg.shape
    size = b.shape[1] // blocks
    columns = cot.shape[1]
    chips = blocks // 2
    anywhere = pl.BlockSpec(memory_space=pl.ANY)
    dma = pltpu.SemaphoreType.DMA
    operands, in_specs = [hg, b, cot, dg, du], [anywhere] * 5
    out_specs = [pl.BlockSpec((size, 3 * columns), lambda p: (jnp.maximum(p - chips, 0), 0))]
    out_shape = [jax.ShapeDtypeStruct((chips * size, 3 * columns), BF)]
    scratch = (
        [pltpu.VMEM(hg.shape, BF)]
        + [pltpu.VMEM((rows, columns), BF)] * 4
        + [pltpu.VMEM((min(chips, SLOTS), size, 3 * columns), BF), pltpu.VMEM((chips, size, 3 * columns), BF)]
        + [dma((5,)), dma((chips,)), dma((chips,))]
    )
    if count:
        own_rows, cols = rows // count, columns // count
        once = pl.Buffered(1)
        operands += [partial, grad] + [dense] * count
        in_specs += [anywhere, pl.BlockSpec(grad.shape, lambda p: (0, 0), pipeline_mode=once)]
        in_specs += [pl.BlockSpec((columns, cols), lambda p, j=j: (0, 3 + j), pipeline_mode=once) for j in range(count)]
        out_specs += [anywhere, anywhere]
        out_shape += [jax.ShapeDtypeStruct((own_rows, columns), BF), jax.ShapeDtypeStruct((rows, cols), BF)]
        scratch += [dma((2,)), pltpu.VMEM((count, own_rows, cols), BF), dma((count - 1,)), dma((count - 1,)), dma]
    return pl.pallas_call(
        functools.partial(grads_kernel, count),
        grid=(blocks,),
        in_specs=in_specs,
        out_specs=out_specs,
        out_shape=out_shape,
        scratch_shapes=scratch,
        compiler_params=pltpu.CompilerParams(
            collective_id=call, has_side_effects=True, vmem_limit_bytes=67043328
        ),
        cost_estimate=SHORT,
        name="grads%d" % call,
    )(*operands)


def pair_kernel(left, right, out, sent, landed, send_sem, recv_sem):
    step = pl.program_id(0)
    group = lax.axis_index("group")
    core, other = lax.rem(group, 2), flipped(group, 1)
    size, chips = out.shape[0], landed.shape[0]

    def copy(chip):
        return pltpu.make_async_remote_copy(
            src_ref=sent.at[chip], dst_ref=landed.at[chip], send_sem=send_sem.at[chip], recv_sem=recv_sem.at[chip],
            device_id={"group": other}, device_id_type=MESH,
        )

    def term(place):
        return dot_tn(left[:, pl.ds(pl.multiple_of(place * size, size), size)], right[...])

    @pl.when(step == 0)
    def _():
        barrier = pltpu.get_barrier_semaphore()
        pl.semaphore_signal(barrier, inc=1, device_id={"group": other}, device_id_type=MESH)
        pl.semaphore_wait(barrier, 1)

    @pl.when(step < chips)
    def _():
        sent[step] = term(2 * step + 1 - core).astype(BF)
        copy(step).start()

    @pl.when(step >= chips)
    def _():
        chip = step - chips
        total = term(2 * chip + core)
        copy(chip).wait_recv()
        out[...] = (total + landed[chip].astype(F32)).astype(BF)

    @pl.when(step == 2 * chips - 1)
    def _():
        for chip in range(chips):
            copy(chip).wait_send()


def pair_terms(left, right, groups, call):
    size, chips = left.shape[1] // groups, groups // 2
    columns = right.shape[1]
    whole = lambda value: pl.BlockSpec(value.shape, lambda p: (0, 0))
    dma = pltpu.SemaphoreType.DMA
    return pl.pallas_call(
        pair_kernel,
        grid=(groups,),
        in_specs=[whole(left), whole(right)],
        out_specs=pl.BlockSpec((size, columns), lambda p: (jnp.maximum(p - chips, 0), 0)),
        out_shape=jax.ShapeDtypeStruct((chips * size, columns), BF),
        scratch_shapes=[pltpu.VMEM((chips, size, columns), BF)] * 2 + [dma((chips,))] * 2,
        compiler_params=pltpu.CompilerParams(collective_id=call, has_side_effects=True),
        cost_estimate=SHORT,
        name="pair%d" % call,
    )(left, right)


def heads_kernel(count, value, out, send_sem, recv_sem, own_sem):
    here = lax.axis_index("expert")
    rows, cols = out.shape[0], value.shape[1]
    others = [lax.rem(here + step, count) for step in range(1, count)]
    barrier = pltpu.get_barrier_semaphore()
    for other in others:
        pl.semaphore_signal(barrier, inc=1, device_id={"expert": other}, device_id_type=MESH)
    pl.semaphore_wait(barrier, count - 1)
    place = out.at[:, pl.ds(pl.multiple_of(here * cols, cols), cols)]

    def block(other):
        return value.at[pl.ds(pl.multiple_of(other * rows, rows), rows)]

    copies = [
        pltpu.make_async_remote_copy(
            src_ref=block(other), dst_ref=place, send_sem=send_sem.at[i], recv_sem=recv_sem.at[i],
            device_id={"expert": other}, device_id_type=MESH,
        )
        for i, other in enumerate(others)
    ]
    for copy in copies:
        copy.start()
    own = pltpu.make_async_copy(block(here), place, own_sem)
    own.start()
    own.wait()
    for copy in copies:
        copy.wait()


def heads_to_rows(value, count, call):
    vmem = pl.BlockSpec(memory_space=pltpu.VMEM)
    dma = pltpu.SemaphoreType.DMA
    return pl.pallas_call(
        functools.partial(heads_kernel, count),
        out_shape=jax.ShapeDtypeStruct((value.shape[0] // count, value.shape[1] * count), value.dtype),
        in_specs=[vmem],
        out_specs=vmem,
        scratch_shapes=[dma((count - 1,)), dma((count - 1,)), dma],
        compiler_params=pltpu.CompilerParams(collective_id=call, has_side_effects=True),
        cost_estimate=SHORT,
        name="heads%d" % call,
    )(value)


def flipped(index, mask):
    bit = 1
    while bit <= mask:
        if mask & bit:
            index = index + bit * (1 - 2 * lax.rem(lax.div(index, bit), 2))
        bit *= 2
    return index


def subsets(bits):
    sums = [0]
    for bit in bits:
        sums = sums + [value + bit for value in sums]
    return sums


def tail_kernel(
    count, groups, grads, weight, hidden, normed, sums, rows_out, *refs
):
    final_outs, sums_out, refs = refs[:3], refs[3], refs[4:]
    (
        query_out, key_out, value_out, final_sem,
        sent, landed, core_out, core_in, held, step_in, done, small, small_in, small_sum,
        all_in, own_sem, token_send, token_recv, core_send, core_recv, step_send, step_recv, whole_send,
        whole_recv, small_send, small_recv, all_send, all_recv,
    ) = refs
    here, group = lax.axis_index("expert"), lax.axis_index("group")
    right, left = lax.rem(here + 1, count), lax.rem(here + count - 1, count)
    others = [lax.rem(here + step, count) for step in range(1, count)]
    bits = [1 << i for i in range(1, groups.bit_length() - 1)]
    orders = (bits, bits[::-1])
    barrier = pltpu.get_barrier_semaphore()
    for other in others:
        pl.semaphore_signal(barrier, inc=1, device_id={"expert": other}, device_id_type=MESH)
    peers = [lax.rem(group + step, groups) for step in range(1, groups)]
    for peer in peers:
        pl.semaphore_signal(barrier, inc=1, device_id={"group": peer}, device_id_type=MESH)
    pl.semaphore_wait(barrier, count + groups - 2)

    rows, width = rows_out.shape
    half = width // 2
    master, columns = held.shape[1:]
    cols = width // count

    def to(axis, other, source, target, send, receive):
        return pltpu.make_async_remote_copy(
            src_ref=source, dst_ref=target, send_sem=send, recv_sem=receive,
            device_id={axis: other}, device_id_type=MESH,
        )

    rest = subsets(bits)

    core = [
        to("group", flipped(group, 1), core_out.at[i], core_in.at[i], core_send.at[i], core_recv.at[i])
        for i in range(len(rest))
    ]
    backward = list(enumerate(rest))[::-1]

    def own_term(block):
        lanes = pl.ds(pl.multiple_of(block * master, master), master)
        return dot_tn(hidden[:, lanes], grads[...])

    def token_block(step, piece):
        block = lax.rem(here - 1 - step + count, count)
        return dot_nt(grads[pl.ds(pl.multiple_of(block * rows, rows), rows), :],
                      weight[piece * half : (piece + 1) * half, :])

    def token_hop(step, piece):
        return to("expert", right, sent.at[step % 2, piece], landed.at[step, piece],
                  token_send.at[step, piece], token_recv.at[step, piece])

    for piece in range(2):
        sent[0, piece] = token_block(0, piece).astype(BF)
        token_hop(0, piece).start()

    def token_step(step):
        terms = [token_block(step, piece) for piece in range(2)]
        for piece in range(2):
            token_hop(step - 1, piece).wait_recv()
            total = terms[piece] + landed[step - 1, piece].astype(F32)
            if step < count - 1:
                if step >= 2:
                    token_hop(step - 2, piece).wait_send()
                sent[step % 2, piece] = total.astype(BF)
                token_hop(step, piece).start()
            else:
                rows_out[:, piece * half : (piece + 1) * half] = total

    def moves(order, level):
        bit = order[level]
        sends = [r for r in rest if r & bit and not r & sum(order[:level])]
        return bit, sends, sum(len(rest) >> (i + 1) for i in range(level))

    outs = (query_out, key_out, value_out)
    pieces = len(outs)

    def whole_hop(step, piece):
        owner = lax.rem(here - step + count, count)
        target = outs[piece].at[:, pl.ds(pl.multiple_of(owner * cols, cols), cols)]
        source = done.at[:, pl.ds(piece * cols, cols)] if step == 0 else target
        return to("expert", right, source, target, whole_send.at[step, piece], whole_recv.at[step, piece])

    own = [
        pltpu.make_async_copy(
            done.at[:, pl.ds(piece * cols, cols)],
            outs[piece].at[:, pl.ds(pl.multiple_of(here * cols, cols), cols)],
            own_sem.at[piece],
        )
        for piece in range(pieces)
    ]

    def whole_start():
        for piece in range(pieces):
            whole_hop(0, piece).start()
        for copy in own:
            copy.start()

    streams = [(slice(0, columns // 2), orders[0]), (slice(columns // 2, columns), orders[1])]

    def step_copies(stream, level):
        lanes, order = streams[stream]
        bit, sends, first = moves(order, level)
        return [
            to("group", flipped(group, bit), held.at[rest.index(r), :, lanes],
               step_in.at[stream, first + i],
               step_send.at[stream, first + i], step_recv.at[stream, first + i])
            for i, r in enumerate(sends)
        ]

    copies = [[step_copies(stream, level) for level in range(len(bits))] for stream in range(2)]
    for i, r in backward:
        core_out[i] = own_term(flipped(group, 1 + r)).astype(BF)
        core[i].start()
    for i, r in backward:
        term = own_term(flipped(group, r))
        core[i].wait_recv()
        held[i] = (term + core_in[i].astype(F32)).astype(BF)
        for stream in range(2):
            sends = moves(streams[stream][1], 0)[1]
            if r in sends:
                copies[stream][0][sends.index(r)].start()

    def reduce_step(level):
        for stream in range(2):
            lanes, order = streams[stream]
            bit, sends, first = moves(order, level)
            for i, r in enumerate(sends):
                copies[stream][level][i].wait()
                kept = rest.index(r - bit)
                total = (held[kept, :, lanes].astype(F32) + step_in[stream, first + i].astype(F32)).astype(BF)
                if level < len(bits) - 1:
                    held[kept, :, lanes] = total
                else:
                    done[:, lanes] = total
            if level < len(bits) - 1:
                for copy in copies[stream][level + 1]:
                    copy.start()

    levels = iter(range(len(bits)))
    for step in range(1, count):
        token_step(step)
        level = next(levels, None)
        if level is not None:
            reduce_step(level)
            if level == len(bits) - 1:
                whole_start()
    small[...] = sums[...]
    small[0:1, :] = jnp.sum(rows_out[...] * normed[...], 0, keepdims=True)
    small_copies = [
        to("group", peer, small.at[:, pl.ds(pl.multiple_of(peer * master, master), master)], small_in.at[i],
           small_send.at[i], small_recv.at[i])
        for i, peer in enumerate(peers)
    ]
    for copy in small_copies:
        copy.start()
    total = small[:, pl.ds(pl.multiple_of(group * master, master), master)]
    for i, copy in enumerate(small_copies):
        copy.wait()
        total = total + small_in[i]
    small_sum[...] = total
    all_copies = [
        to("expert", other, small_sum, all_in.at[i], all_send.at[i], all_recv.at[i]) for i, other in enumerate(others)
    ]
    for copy in all_copies:
        copy.start()
    for step in range(1, count - 1):
        for piece in range(pieces):
            whole_hop(step - 1, piece).wait_recv()
            whole_hop(step, piece).start()
    for i, copy in enumerate(all_copies):
        copy.wait()
        total = total + all_in[i]
    sums_out[...] = total
    for piece in range(pieces):
        own[piece].wait()
        whole_hop(count - 2, piece).wait_recv()
    finals = [
        pltpu.make_async_copy(source, target, final_sem.at[i])
        for i, (source, target) in enumerate(zip((query_out, key_out, value_out), final_outs))
    ]
    for copy in finals:
        copy.start()
    for copy in core:
        copy.wait_send()
    for step in range(count - 1):
        if step >= count - 3:
            for piece in range(2):
                token_hop(step, piece).wait_send()
        for piece in range(pieces):
            whole_hop(step, piece).wait_send()
    for copy in finals:
        copy.wait()


def tail(grads, dense, hidden, normed, sums, count, groups, call):
    rows, width = hidden.shape[0] // count, hidden.shape[1]
    own_columns = grads.shape[1]
    master = width // groups
    rest = groups // 2
    dma = pltpu.SemaphoreType.DMA
    vmem = pl.BlockSpec(memory_space=pltpu.VMEM)
    return pl.pallas_call(
        functools.partial(tail_kernel, count, groups),
        out_shape=[jax.ShapeDtypeStruct((rows, width), F32)] + [jax.ShapeDtypeStruct((master, width), BF)] * 3
        + [jax.ShapeDtypeStruct((sums.shape[0], master), F32)],
        grid=(1,),
        in_specs=[
            pl.BlockSpec(grads.shape, lambda i: (0, 0)),
            pl.BlockSpec((width, own_columns), lambda i: (0, 0)),
            pl.BlockSpec(hidden.shape, lambda i: (0, 0)),
            pl.BlockSpec(normed.shape, lambda i: (0, 0)),
            pl.BlockSpec(sums.shape, lambda i: (0, 0)),
        ],
        out_specs=[vmem] + [pl.BlockSpec(memory_space=pl.ANY)] * 3 + [vmem],
        scratch_shapes=[pltpu.VMEM((master, width), BF)] * 3
        + [
            dma((3,)),
            pltpu.VMEM((2, 2, rows, width // 2), BF),
            pltpu.VMEM((count - 1, 2, rows, width // 2), BF),
            pltpu.VMEM((rest, master, own_columns), BF),
            pltpu.VMEM((rest, master, own_columns), BF),
            pltpu.VMEM((rest, master, own_columns), BF),
            pltpu.VMEM((2, rest - 1, master, own_columns // 2), BF),
            pltpu.VMEM((master, own_columns), BF),
            pltpu.VMEM(sums.shape, F32),
            pltpu.VMEM((groups - 1, sums.shape[0], master), F32),
            pltpu.VMEM((sums.shape[0], master), F32),
            pltpu.VMEM((count - 1, sums.shape[0], master), F32),
            dma((3,)),
            dma((count - 1, 2)),
            dma((count - 1, 2)),
            dma((rest,)),
            dma((rest,)),
            dma((2, rest - 1)),
            dma((2, rest - 1)),
            dma((count - 1, 3)),
            dma((count - 1, 3)),
        ]
        + [dma((groups - 1,))] * 2
        + [dma((count - 1,))] * 2,
        compiler_params=pltpu.CompilerParams(
            collective_id=call, has_side_effects=True, vmem_limit_bytes=67043328
        ),
        cost_estimate=SHORT,
        name="tail",
    )(grads, dense, hidden, normed, sums)


def finish_kernel(*refs):
    in1, down1a, down1b, in2, down2a, down2b = refs[:6]
    dense, (out_in, out_down), dense_out = refs[6:10], refs[10:12], refs[12:]
    ff = out_in.shape[2] // 2
    for pair, value in enumerate((in1, in2)):
        for part in range(2):
            for j in range(PAIR):
                at = (PAIR * (1 + part) + j) * ff
                out_in[:, pair * PAIR + j, part * ff : (part + 1) * ff] = value[:, at : at + ff].astype(F32)
    for i, value in enumerate((down1a, down1b, down2a, down2b)):
        out_down[:, i, :] = value[...].astype(F32)
    for value, out in zip(dense, dense_out):
        out[...] = value[...].astype(F32)


def finish_grads(sum1, sum2, dense):
    master, columns = sum1.shape
    width = columns // 3
    steps = master // PREP_ROWS
    rows = PREP_ROWS // PAIR
    local = 2 * PAIR
    specs = [pl.BlockSpec((PREP_ROWS, columns), lambda i: (i, 0))]
    specs += [pl.BlockSpec((rows, width), lambda i, j=j: (j * steps + i, 0)) for j in range(PAIR)]
    whole = [pl.BlockSpec((PREP_ROWS, width), lambda i: (i, 0))] * len(dense)
    return pl.pallas_call(
        finish_kernel,
        grid=(steps,),
        in_specs=specs * 2 + whole,
        out_specs=[
            pl.BlockSpec((PREP_ROWS, local, width), lambda i: (i, 0, 0)),
            pl.BlockSpec((rows, local, width), lambda i: (i, 0, 0)),
        ]
        + whole,
        out_shape=[
            jax.ShapeDtypeStruct((master, local, width), F32),
            jax.ShapeDtypeStruct((master // PAIR, local, width), F32),
        ]
        + [jax.ShapeDtypeStruct((master, width), F32)] * len(dense),
        cost_estimate=SHORT,
        name="finish",
    )(sum1, sum1, sum1, sum2, sum2, sum2, *dense)


def key_limit(block):
    return max((block + 1) * QBLOCK, MAX_PREFIX)


def visible(block, limit, prefix):
    row = block * QBLOCK + lax.broadcasted_iota(jnp.int32, (QBLOCK, limit), 0)
    col = lax.broadcasted_iota(jnp.int32, (QBLOCK, limit), 1)
    return (col <= row) | (col < prefix)


def attend_kernel(prefix_ref, ql, kl, vb, sq, sk, gq, gk, cos, sin, ob, qb, kb, lse):
    prefix = prefix_ref[0]
    c, s = cos[...], sin[...]
    qn = ql[...] * sq[...] * gq[...]
    kn = kl[...] * sk[...] * gk[...]
    half = HEAD_DIM // 2
    qb[...] = ((qn * c + pltpu.roll(qn, half, 1) * s) * HEAD_DIM ** (-0.5)).astype(BF)
    kb[...] = (kn * c + pltpu.roll(kn, half, 1) * s).astype(BF)
    for block in range(LEN // QBLOCK):
        rows = slice(block * QBLOCK, (block + 1) * QBLOCK)
        limit = key_limit(block)
        scores = dot_nt(qb[rows, :], kb[:limit, :])
        scores = jnp.where(visible(block, limit, prefix), scores, -1e30)
        peak = jnp.max(scores, -1, keepdims=True)
        expo = jnp.exp(scores - peak)
        total = jnp.sum(expo, -1, keepdims=True)
        ob[rows, :] = (dot(expo.astype(BF), vb[:limit, :]) / total).astype(BF)
        lse[0, rows, :] = peak + jnp.log(total)


def attend(prefix, ql, kl, vb, sq, sk, gq, gk, cos, sin):
    heads = ql.shape[1] // HEAD_DIM
    col = pl.BlockSpec((LEN, HEAD_DIM), lambda h, p: (0, h))
    one = pl.BlockSpec((LEN, 1), lambda h, p: (0, 0))
    gain = pl.BlockSpec((1, HEAD_DIM), lambda h, p: (0, h))
    table = pl.BlockSpec((LEN, HEAD_DIM), lambda h, p: (0, 0))
    return pl.pallas_call(
        attend_kernel,
        out_shape=[jax.ShapeDtypeStruct(ql.shape, BF)] * 3
        + [jax.ShapeDtypeStruct((heads, LEN, 1), F32)],
        grid_spec=pltpu.PrefetchScalarGridSpec(
            num_scalar_prefetch=1,
            grid=(heads,),
            in_specs=[col, col, col, one, one, gain, gain, table, table],
            out_specs=[col, col, col, pl.BlockSpec((1, LEN, 1), lambda h, p: (h, 0, 0))],
        ),
        cost_estimate=SHORT,
        name="attend",
    )(prefix, ql, kl, vb, sq, sk, gq, gk, cos, sin)


def attend_back_kernel(
    prefix_ref, qb, kb, vb, dob, lse, ql, kl, sq, sk, gq, gk, cos, sin,
    wq, wk, dv, inner, gain_q, gain_k, dq_sum, dk_sum, dv_sum,
):
    prefix = prefix_ref[0]
    dk_sum[...] = jnp.zeros_like(dk_sum)
    dv_sum[...] = jnp.zeros_like(dv_sum)
    for block in range(LEN // QBLOCK):
        rows = slice(block * QBLOCK, (block + 1) * QBLOCK)
        limit = key_limit(block)
        scores = dot_nt(qb[rows, :], kb[:limit, :])
        weights = jnp.where(visible(block, limit, prefix), jnp.exp(scores - lse[0, rows, :]), 0.0)
        grad = dob[rows, :]
        dweights = dot_nt(grad, vb[:limit, :])
        dscores = (weights * (dweights - jnp.sum(dweights * weights, -1, keepdims=True))).astype(BF)
        dq_sum[rows, :] = dot(dscores, kb[:limit, :])
        dk_sum[:limit, :] += dot_tn(dscores, qb[rows, :])
        dv_sum[:limit, :] += dot_tn(weights.astype(BF), grad)
    dv[...] = dv_sum[...].astype(BF)
    c, s = cos[...], sin[...]
    half = HEAD_DIM // 2
    dq = dq_sum[...] * HEAD_DIM ** (-0.5)
    dqn = dq * c - pltpu.roll(dq, half, 1) * s
    dk = dk_sum[...]
    dkn = dk * c - pltpu.roll(dk, half, 1) * s
    gain_q[...] = jnp.sum(dqn * (ql[...] * sq[...]), 0, keepdims=True)
    gain_k[...] = jnp.sum(dkn * (kl[...] * sk[...]), 0, keepdims=True)
    dqn = dqn * gq[...]
    dkn = dkn * gk[...]
    wq[...] = dqn
    wk[...] = dkn
    part = jnp.concatenate(
        [jnp.sum(dqn * ql[...], -1, keepdims=True), jnp.sum(dkn * kl[...], -1, keepdims=True)], 1
    )

    @pl.when(pl.program_id(0) == 0)
    def _():
        inner[...] = part

    @pl.when(pl.program_id(0) > 0)
    def _():
        inner[...] += part


def attend_back(prefix, qb, kb, vb, dob, lse, ql, kl, sq, sk, gq, gk, cos, sin):
    heads = ql.shape[1] // HEAD_DIM
    col = pl.BlockSpec((LEN, HEAD_DIM), lambda h, p: (0, h))
    one = pl.BlockSpec((LEN, 1), lambda h, p: (0, 0))
    gain = pl.BlockSpec((1, HEAD_DIM), lambda h, p: (0, h))
    table = pl.BlockSpec((LEN, HEAD_DIM), lambda h, p: (0, 0))
    return pl.pallas_call(
        attend_back_kernel,
        out_shape=[
            jax.ShapeDtypeStruct(ql.shape, F32),
            jax.ShapeDtypeStruct(ql.shape, F32),
            jax.ShapeDtypeStruct(ql.shape, BF),
            jax.ShapeDtypeStruct((LEN, 2), F32),
            jax.ShapeDtypeStruct((1, ql.shape[1]), F32),
            jax.ShapeDtypeStruct((1, ql.shape[1]), F32),
        ],
        grid_spec=pltpu.PrefetchScalarGridSpec(
            num_scalar_prefetch=1,
            grid=(heads,),
            in_specs=[col, col, col, col, pl.BlockSpec((1, LEN, 1), lambda h, p: (h, 0, 0)),
                      col, col, one, one, gain, gain, table, table],
            out_specs=[col, col, col, pl.BlockSpec((LEN, 2), lambda h, p: (0, 0)), gain, gain],
            scratch_shapes=[pltpu.VMEM((LEN, HEAD_DIM), F32)] * 3,
        ),
        cost_estimate=SHORT,
        name="attend_back",
    )(prefix, qb, kb, vb, dob, lse, ql, kl, sq, sk, gq, gk, cos, sin)


FTILE = 256
PAIR = 2


def expert_kernel(first, b, c, wg, wu, wd, gates, hg, dg, du, dgate):
    lanes = lax.broadcasted_iota(jnp.int32, gates.shape, 1) == first[0] + pl.program_id(0)
    g = dot(b[...], wg[...])
    u = dot(b[...], wu[...])
    back = dot_nt(c[...], wd[...].reshape(FTILE, wd.shape[-1]))
    sigma = jax.nn.sigmoid(g)
    silu = g * sigma
    h = silu * u
    weight = jnp.sum(jnp.where(lanes, gates[...], 0.0), -1, keepdims=True)
    hidden = (weight * h).astype(BF)
    block = hg.shape[3]
    for i in range(hg.shape[0]):
        hg[i, 0] = hidden[:, i * block : (i + 1) * block]
    part = jnp.where(lanes, jnp.sum(h * back, -1, keepdims=True), 0.0)
    dh = weight * back
    dg[...] = (dh * u * (sigma * (1.0 + g * (1.0 - sigma)))).astype(BF)
    du[...] = (dh * silu).astype(BF)
    start = (pl.program_id(0) == 0) & (pl.program_id(1) == 0)

    @pl.when(start)
    def _():
        dgate[...] = part

    @pl.when(jnp.logical_not(start))
    def _():
        dgate[...] += part


def experts(first, b, c, weights, gates, ff):
    rows, width = b.shape
    tiles = ff // FTILE
    block = weights.shape[2]
    whole = pl.BlockSpec((rows, width), lambda j, f, p: (0, 0), pipeline_mode=pl.Buffered(1))
    one = pl.BlockSpec((rows, LANES), lambda j, f, p: (0, 0))
    out = pl.BlockSpec((rows, FTILE), lambda j, f, p: (0, j * tiles + f))
    flat = weights.reshape(width, weights.shape[3])
    return pl.pallas_call(
        expert_kernel,
        grid_spec=pltpu.PrefetchScalarGridSpec(
            num_scalar_prefetch=1,
            grid=(PAIR, tiles),
            in_specs=[
                whole,
                whole,
                pl.BlockSpec((width, FTILE), lambda j, f, p: (0, j * tiles + f)),
                pl.BlockSpec((width, FTILE), lambda j, f, p: (0, (PAIR + j) * tiles + f)),
                pl.BlockSpec((FTILE // block, 1, block, width), lambda j, f, p: (f, j, 0, 2)),
                one,
            ],
            out_specs=[
                pl.BlockSpec((FTILE // block, 1, rows, block), lambda j, f, p: (f, j, 0, 0)),
                out,
                out,
                one,
            ],
        ),
        out_shape=[jax.ShapeDtypeStruct((ff // block, PAIR, rows, block), BF)]
        + [jax.ShapeDtypeStruct((rows, PAIR * ff), BF)] * 2
        + [jax.ShapeDtypeStruct((rows, LANES), F32)],
        cost_estimate=SHORT,
        name="experts",
    )(first, b, c, flat, flat, weights, gates)


NTILE = 256
GROUPS = 8
STEP_BACK, STEP_DOWN, LINK_US, HOP_US = 5.4, 2.8, 2.85, 3.5


def ring_steps(count, tiles, last):
    per = tiles // GROUPS
    ends, now = [], 0.0
    for step in range(last + 1):
        now += STEP_BACK if step < tiles else STEP_DOWN
        ends.append(now)
    steps, ready, free = {}, {(GROUPS, 0): 0.0}, 0.0
    pending = []
    for step in range(last + 1):
        if step < tiles and step % per == per - 1:
            ready[step // per, 0] = ends[step]
        while ready:
            action = min(ready, key=lambda key: (ready[key], key))
            if ready[action] > ends[step] and step < last:
                break
            at = max(ready.pop(action), ends[step])
            steps.setdefault(step, []).append(action)
            group, hop = action
            if hop < count - 1:
                free = max(free, at) + LINK_US
                ready[group, hop + 1] = free + HOP_US
    return steps


def middle_kernel(
    count, tiles, steps, dg1, du1, dg2, du2, hg1, hg2, probs, wg1, wu1, wg2, wu2, wd1, wd2,
    back_out, partial,
    held1, held2, held3, held4, hidden1, hidden2, back, sent, landed, probs_sent, probs_landed,
    load_sem, send_sem, recv_sem,
):
    step = pl.program_id(0)
    here = lax.axis_index("expert")
    right, left = lax.rem(here + 1, count), lax.rem(here + count - 1, count)
    columns = tiles * NTILE
    lanes = columns // GROUPS
    rows = back.shape[0] // count
    loads = [
        pltpu.make_async_copy(source, target, load_sem.at[i])
        for i, (source, target) in enumerate(
            (
                (dg1, held1), (du1, held2), (dg2, held3), (du2, held4),
                (hg1, hidden1), (hg2, hidden2),
            )
        )
    ]

    @pl.when(step == 0)
    def _():
        barrier = pltpu.get_barrier_semaphore()
        for other in (left, right):
            pl.semaphore_signal(barrier, inc=1, device_id={"expert": other}, device_id_type=MESH)
        for load in loads:
            load.start()
        pl.semaphore_wait(barrier, 2)
        total = None
        for i, (left_ref, right_ref) in enumerate(((held1, wg1), (held2, wu1), (held3, wg2), (held4, wu2))):
            loads[i].wait()
            term = dot_nt(left_ref[...], right_ref[...])
            total = term if total is None else total + term
        back[:, :NTILE] = total.astype(BF)

    @pl.when((step > 0) & (step < tiles))
    def _():
        total = (
            dot_nt(held1[...], wg1[...])
            + dot_nt(held2[...], wu1[...])
            + dot_nt(held3[...], wg2[...])
            + dot_nt(held4[...], wu2[...])
        )
        back[:, pl.ds(pl.multiple_of(step * NTILE, NTILE), NTILE)] = total.astype(BF)

    @pl.when(step == tiles)
    def _():
        loads[4].wait()
        loads[5].wait()

    @pl.when(step >= tiles)
    def _():
        total = None
        for hidden, weight in ((hidden1, wd1), (hidden2, wd2)):
            for j in range(PAIR):
                left_value = jnp.concatenate([hidden[i, j] for i in range(hidden.shape[0])], -1)
                term = dot(left_value, weight[:, j].reshape(left_value.shape[1], NTILE))
                total = term if total is None else total + term
        partial[...] = total.astype(BF)

    def copy(group, hop):
        source, target = (sent, landed) if group < GROUPS else (probs_sent, probs_landed)
        at = (hop, group) if group < GROUPS else (hop,)
        return pltpu.make_async_remote_copy(
            src_ref=source.at[at], dst_ref=target.at[at],
            send_sem=send_sem.at[hop, group], recv_sem=recv_sem.at[hop, group],
            device_id={"expert": right}, device_id_type=MESH,
        )

    def advance(group, hop):
        at = (slice(group * lanes, (group + 1) * lanes) if group < GROUPS else slice(columns, columns + LANES))
        block = pl.ds(pl.multiple_of(lax.rem(here - 1 - hop + count, count) * rows, rows), rows)
        total = (back[block, at] if group < GROUPS else probs[block, :]).astype(F32)
        if hop:
            copy(group, hop - 1).wait_recv()
            total = total + (landed[hop - 1, group] if group < GROUPS else probs_landed[hop - 1]).astype(F32)
        if hop == count - 1:
            back_out[:, at] = total
            return
        if group < GROUPS:
            sent[hop, group] = total.astype(BF)
        else:
            probs_sent[hop] = total.astype(BF)
        copy(group, hop).start()

    for at, actions in steps.items():

        @pl.when(step == at)
        def _():
            for group, hop in actions:
                advance(group, hop)

    @pl.when(step == pl.num_programs(0) - 1)
    def _():
        for hop in range(count - 1):
            for group in range(GROUPS + 1):
                copy(group, hop).wait_send()


def middle(pair1, pair2, probs, weights1, weights2, count, call):
    (hg1, dg1, du1), (hg2, dg2, du2) = pair1, pair2
    devices, _, rows, block = hg1.shape
    width = devices * PAIR * block
    tiles = width // NTILE
    flat1, flat2 = [w.reshape(width, w.shape[3]) for w in (weights1, weights2)]
    anywhere = pl.BlockSpec(memory_space=pl.ANY)
    gate = pl.BlockSpec((NTILE, width), lambda s: (jnp.minimum(s, tiles - 1), 0))
    up = pl.BlockSpec((NTILE, width), lambda s: (jnp.minimum(s, tiles - 1), 1))
    second = lambda s: jnp.clip(s - tiles, 0, tiles - 1)
    weight = pl.BlockSpec((devices, PAIR, block, NTILE), lambda s: (0, 0, 0, 2 * width // NTILE + second(s)))
    dma = pltpu.SemaphoreType.DMA
    lanes = width // GROUPS
    return pl.pallas_call(
        functools.partial(middle_kernel, count, tiles, ring_steps(count, tiles, 2 * tiles - 1)),
        grid=(2 * tiles,),
        in_specs=[anywhere] * 6
        + [pl.BlockSpec((rows, LANES), lambda s: (0, 0), pipeline_mode=pl.Buffered(1))]
        + [gate, up, gate, up, weight, weight],
        out_specs=[
            pl.BlockSpec((rows // count, width + LANES), lambda s: (0, 0), pipeline_mode=pl.Buffered(1)),
            pl.BlockSpec((rows, NTILE), lambda s: (0, second(s))),
        ],
        out_shape=[
            jax.ShapeDtypeStruct((rows // count, width + LANES), F32),
            jax.ShapeDtypeStruct((rows, width), BF),
        ],
        scratch_shapes=[pltpu.VMEM((rows, width), BF)] * 4
        + [pltpu.VMEM(hg1.shape, BF)] * 2
        + [
            pltpu.VMEM((rows, width), BF),
            pltpu.VMEM((count - 1, GROUPS, rows // count, lanes), BF),
            pltpu.VMEM((count - 1, GROUPS, rows // count, lanes), BF),
            pltpu.VMEM((count - 1, rows // count, LANES), BF),
            pltpu.VMEM((count - 1, rows // count, LANES), BF),
            dma((6,)),
            dma((count - 1, GROUPS + 1)),
            dma((count - 1, GROUPS + 1)),
        ],
        compiler_params=pltpu.CompilerParams(
            collective_id=call, has_side_effects=True, vmem_limit_bytes=67043328
        ),
        cost_estimate=SHORT,
        name="middle",
    )(dg1, du1, dg2, du2, hg1, hg2, probs, flat1, flat1, flat2, flat2, weights1, weights2)


def body(
    tokens,
    routes,
    prefix,
    query_weight,
    key_weight,
    value_weight,
    output_weight,
    router_weight,
    attention_gain,
    feedforward_gain,
    query_gain,
    key_gain,
    expert_in,
    expert_down,
    cotangent,
):
    count = lax.axis_size("expert")
    here = lax.axis_index("expert")
    rows, width = tokens.shape
    cols = width // count
    experts_all = router_weight.shape[1]
    local = expert_in.shape[1]
    ff_rows = expert_down.shape[0]
    ff = expert_in.shape[2] // 2
    master = query_weight.shape[0]

    def gather(value):
        return lax.all_gather(value, "group", axis=0, tiled=True)

    cores = [list(range(core, width // master, 2)) for core in range(2)]

    def scatter(value):
        return lax.psum_scatter(value, "group", scatter_dimension=0, tiled=True, axis_index_groups=cores)

    def own_cols(weight):
        return lax.dynamic_slice(weight, (0, here * cols), (master, cols)).astype(BF)

    small = jnp.concatenate(
        [
            jnp.pad(router_weight, ((0, 0), (0, LANES // 2 - experts_all))),
            jnp.stack([attention_gain, feedforward_gain, query_gain, key_gain], 1),
            jnp.zeros((master, LANES // 2 - 4), F32),
        ],
        1,
    ).astype(BF)
    dense = gather(
        jnp.concatenate(
            [own_cols(query_weight), own_cols(key_weight), own_cols(value_weight), output_weight.astype(BF), small],
            1,
        )
    )
    qkv_weight = dense[:, : 3 * cols]
    out_weight = dense[:, 3 * cols : 3 * cols + width]
    router = dense[:, 3 * cols + width :]
    gains = router[:, LANES // 2 :].astype(F32).T
    gain_one, gain_two = gains[0:1], gains[1:2]
    gain_query = lax.dynamic_slice(gains[2:3], (0, here * cols), (1, cols))
    gain_key = lax.dynamic_slice(gains[3:4], (0, here * cols), (1, cols))

    expert_ids = jnp.arange(experts_all, dtype=jnp.int32)
    selected = jnp.sum((routes[:, :, None] == expert_ids).astype(F32), 1)
    sent = jnp.concatenate(
        [tokens, jnp.pad(selected, ((0, 0), (0, LANES - experts_all))).astype(BF)], 1
    )
    sent, own1, own2 = gather_and_prep(sent, expert_in, expert_down, count, 2)
    weights1, weights2 = [gather(own).reshape(-1, PAIR, ff_rows, own.shape[1]) for own in (own1, own2)]
    x_all = sent[:, :width].astype(F32)
    chosen = sent[:, width:].astype(F32)

    steps = jnp.arange(HEAD_DIM // 2).astype(F32)
    freq = jnp.exp(steps * (-2.0 * math.log(THETA) / HEAD_DIM))
    angle = jnp.arange(LEN).astype(F32)[:, None] * freq[None, :]
    cosine = jnp.concatenate([jnp.cos(angle)] * 2, 1)
    sine = jnp.concatenate([-jnp.sin(angle), jnp.sin(angle)], 1)

    hidden_one = (x_all * row_scale(x_all) * gain_one).astype(BF)
    cot_blocks = [cotangent]

    def cot_hop(value, *done):
        if len(cot_blocks) < count:
            cot_blocks.append(shift(after(cot_blocks[-1], *done), count, 1))
            value = after(value, cot_blocks[-1])
        return value

    hidden_one = cot_hop(hidden_one, sent)
    qkv = dot(hidden_one, qkv_weight)
    query_lin, key_lin = qkv[:, :cols], qkv[:, cols : 2 * cols]
    value_bf = qkv[:, 2 * cols :].astype(BF)
    value_bf = cot_hop(value_bf)
    squares = jnp.stack([jnp.sum(query_lin * query_lin, -1), jnp.sum(key_lin * key_lin, -1)])
    scales = exchange_sum(after(squares, value_bf), count, 0)
    between = scales
    scales = lax.rsqrt(scales / width + EPS)
    scale_query, scale_key = scales[0][:, None], scales[1][:, None]
    attended, query_bf, key_bf, lse = attend(
        prefix, query_lin, key_lin, value_bf, scale_query, scale_key, gain_query, gain_key, cosine, sine
    )
    attended_bf = heads_to_rows(cot_hop(attended, between), count, 4)

    xfloat = tokens.astype(F32)
    resid = xfloat + dot(attended_bf, out_weight)
    scale_two = row_scale(resid)
    normed_two = resid * scale_two
    hidden_two = (normed_two * gain_two).astype(BF)
    while len(cot_blocks) < count:
        hidden_two = cot_hop(hidden_two, attended_bf)
    b_all, = gather_rows((hidden_two,), count, 3)
    cot_all = jnp.zeros((LEN, width), BF)
    for step, block in enumerate(cot_blocks):
        cot_all = lax.dynamic_update_slice(cot_all, block, (((here - step) % count) * rows, 0))

    def route(value):
        lanes = lax.broadcasted_iota(jnp.int32, (1, LANES), 1)
        return jax.nn.softmax(jnp.where(lanes < experts_all, dot(value, router), -1e30), -1)

    gates = route(b_all) * chosen
    own_probs = route(hidden_two)
    first = jnp.full((1,), here * local, jnp.int32)
    devices = width // master
    hg1, dg1, du1, dgate1 = experts(first, b_all, cot_all, weights1, gates, ff)
    term1, = grad_terms(hg1, b_all, cot_all, dg1, du1, 9)
    sum1 = scatter(term1)
    hg2, dg2, du2, dgate2 = experts(first + PAIR, after(b_all, term1), cot_all, weights2, gates, ff)
    dprobs = (dgate1 + dgate2) * chosen

    back, partial = middle((hg1, dg1, du1), (hg2, dg2, du2), dprobs, weights1, weights2, count, 8)
    back = after(back, sum1)
    grad_probs = back[:, width:]
    grad_logits = (
        own_probs * (grad_probs - jnp.sum(grad_probs * own_probs, -1, keepdims=True))
    ).astype(BF)
    grad_router = dot_tn(grad_logits, hidden_two)[:experts_all]
    grad_two = back[:, :width] + dot_nt(grad_logits, router)
    gain_two_term = jnp.sum(grad_two * normed_two, 0)
    grad_out = cotangent.astype(F32)
    grad_resid = grad_out + norm_back(resid, scale_two, grad_two * gain_two)
    grad_attn_out = grad_resid.astype(BF)
    output_term = pair_terms(attended_bf, grad_attn_out, devices, 12)
    output_sum = scatter(output_term)
    term2, first_out, heads_grad = grad_terms(
        hg2, b_all, cot_all, dg2, after(du2, output_term), 10, partial, grad_attn_out, dense, count
    )
    sum2 = scatter(term2)
    ring_out = Ring(partial, first_out, count, here)
    output_sum = lax.psum(after(output_sum, heads_grad), "expert")

    wq, wk, dvl, inner, gain_q_term, gain_k_term = attend_back(
        prefix, query_bf, key_bf, value_bf, heads_grad, lse, query_lin, key_lin,
        scale_query, scale_key, gain_query, gain_key, cosine, sine,
    )
    last = ring_out.hop(inner)
    inner = exchange_sum(after(inner, last).T, count, 1) / width
    ring_out.total = after(ring_out.total, inner)
    dql = scale_query * wq - query_lin * (scale_query**3 * inner[0][:, None])
    dkl = scale_key * wk - key_lin * (scale_key**3 * inner[1][:, None])
    dqkv = jnp.concatenate([dql.astype(BF), dkl.astype(BF), dvl], 1)

    def spread(value):
        return lax.dynamic_update_slice(jnp.zeros((1, width), F32), value, (0, here * cols))

    scale_one = row_scale(xfloat)
    sums = jnp.concatenate(
        [
            jnp.zeros((1, width), F32),
            gain_two_term[None],
            spread(gain_q_term),
            spread(gain_k_term),
            jnp.zeros((4, width), F32),
            grad_router,
        ]
    )
    grad_hidden, *dense_grads, sums = tail(
        dqkv, dense, hidden_one, xfloat * scale_one, sums, count, devices, 6
    )

    output = (resid + ring_out.finish(grad_hidden)).astype(BF)
    grad_tokens = grad_resid + norm_back(xfloat, scale_one, grad_hidden * gain_one)
    grad_in, grad_down, grad_q, grad_k, grad_v, grad_out_weight = finish_grads(
        sum1, sum2, [*dense_grads, output_sum]
    )
    return (
        output,
        grad_tokens,
        grad_q,
        grad_k,
        grad_v,
        grad_out_weight,
        sums[8:].T,
        sums[0],
        sums[1],
        sums[2],
        sums[3],
        grad_in,
        grad_down,
    )


def solution(mesh):
    in_specs = (
        P(("group", "expert"), None),
        P(("group", "expert"), None),
        P("group"),
        P("group", None),
        P("group", None),
        P("group", None),
        P("group", None),
        P("group", None),
        P("group"),
        P("group"),
        P("group"),
        P("group"),
        P("group", "expert", None),
        P("group", "expert", None),
        P(("group", "expert"), None),
    )
    out_specs = (
        P(("group", "expert"), None),
        P(("group", "expert"), None),
        P("group", None),
        P("group", None),
        P("group", None),
        P("group", None),
        P("group", None),
        P("group"),
        P("group"),
        P("group"),
        P("group"),
        P("group", "expert", None),
        P("group", "expert", None),
    )
    return jax.shard_map(body, mesh=mesh, in_specs=in_specs, out_specs=out_specs, check_vma=False)
```
